512 devices in a mesh: groups: 2 (over y), expert: 32 (over z), tensor: 8 (over x, core).
Axes of the slice: x: 4, y: 2, z: 32, core: 2. Of those that a mesh axis runs over, the one named last changes fastest.
The devices are a block of a 4x8x32 slice.
Arguments:
- tokens: bfloat16 [2048, 4096], P(('groups', 'expert')), parts along dimension 0, may hold values from -6 to 6
- route_ids: int32 [2048, 2], P(('groups', 'expert')), parts along dimension 0, may hold values from 0 to 3, all different within a row; in each aligned block of 32 rows (0 to 31, 32 to 63, ...) at most 24 rows name the same one
- route_gates: float32 [2048, 2], P(('groups', 'expert')), parts along dimension 0, may hold values from 0.1 to 1
- gate_weight: bfloat16 [4096, 32768], P(None, ('expert', 'tensor')), may hold values from -0.09375 to 0.09375
- up_weight: bfloat16 [4096, 32768], P(None, ('expert', 'tensor')), may hold values from -0.09375 to 0.09375
- down_weight: bfloat16 [32768, 4096], P('expert', 'tensor'), may hold values from -0.0625 to 0.0625
Outputs:
- mixed: bfloat16 [2048, 4096], P(('groups', 'expert'), 'tensor'), parts along dimension 0
The draws below stay inside these ranges and needn't reach their ends.
There are 2 independent parts, one for each index of `groups`. The reference program is written for one: setup_inputs(seed, part) draws one part's arguments, and reference() takes and returns one part's arrays. A program takes and returns all parts, laid end to end along the dimension named above; an argument that names none is the same for every part. Nothing has to cross between parts.
Inputs may be any that keep to these rules, and one draw needn't show every extreme that they name: `route_ids`: each row names 2 different experts. In the rows of one device no expert is named more than 24 times, and in some device's rows one expert is named exactly 24 times.
All inputs are finite; a program needn't handle non-finite values.
Results may differ from the reference program's by a relative error of at most 0.005.
Values may be sent and summed in bfloat16 or wider, within the bound.
No kernel may reach another device: no remote copies, remote signals or barrier semaphores. Data moves between devices by JAX's collectives and lax.ppermute only.
A program may use at most 64 MiB of HBM per device.

```python
import math
import jax
import jax.numpy as jnp
import numpy as np
from jax import lax

D = 4096
FF = 8192
EXPERTS = 4
TOP = 2
TOK_DEV = 32
CAP = 24
TOKENS = 1024


def levels(rng, shape, shards, least, high):
    gain = 1.0
    for axis_at, parts in shards:
        steps = jax.random.uniform(jax.random.fold_in(jax.random.fold_in(rng, 6), axis_at), (parts,), jnp.float32, least / len(shards), high / len(shards))
        gain = gain * jnp.repeat(jnp.exp(steps), shape[axis_at] // parts).reshape((-1,) + (1,) * (len(shape) - 1 - axis_at))
    return gain


def deal_out(rng, own, number, rows, number_of, top, limit, slope):
    ranking = jax.random.permutation(rng, number_of)
    crowded, ordinary = portions_of(number_of, rows * top, limit, slope, True), portions_of(number_of, rows * top, limit, slope, False)
    places = jnp.arange(number_of)

    def named(sizes, offset_by):
        used = int((sizes > 0).sum())
        fixed = max(1, used // 4)
        passed = fixed + (places - fixed + offset_by * (used - fixed)) % max(1, number_of - fixed)
        return jnp.zeros((number_of,), jnp.int32).at[ranking[jnp.where(places < fixed, places, passed)]].set(jnp.asarray(sizes, jnp.int32))

    sizes = jnp.where(number % 4 == 0, named(crowded, number // 4), named(ordinary, number - number // 4 - 1))
    mixed = jax.random.permutation(jax.random.fold_in(own, 3), number_of)
    giver, sink = mixed[0:number_of // 2 * 2:2], mixed[1:number_of // 2 * 2:2]
    slack = jnp.minimum(sizes[giver] - 1, limit - sizes[sink]) // 2
    slack = jnp.where((giver == ranking[0]) | (sink == ranking[0]) | (sizes[sink] == 0), 0, jnp.maximum(slack, 0))
    passed = jax.random.randint(jax.random.fold_in(own, 4), (number_of // 2,), 0, 1 << 20) % (slack + 1)
    sizes = sizes.at[giver].add(-passed).at[sink].add(passed)
    items = jnp.searchsorted(jnp.cumsum(sizes), jnp.arange(rows * top), side="right").astype(jnp.int32)
    grid = items.reshape(top, rows).T
    grid = grid[jax.random.permutation(jax.random.fold_in(own, 1), rows)]
    offset_by = jax.random.randint(jax.random.fold_in(own, 2), (rows, 1), 0, top)
    return jnp.take_along_axis(grid, (jnp.arange(top)[None, :] + offset_by) % top, axis=1)


def portions_of(amount, total, bound, slope, full):
    portions = [(1 << 20) // math.isqrt(rank ** slope) + 1 for rank in range(1, amount + 1)]
    largest = bound if full else min(bound, max(-(-total // amount), total * portions[0] // sum(portions)))
    least = 1 if total - largest >= amount - 1 else 0
    holding, surplus = [largest] + [least] * (amount - 1), total - largest - least * (amount - 1)
    while surplus > 0:
        free = [i for i in range(1, amount) if holding[i] < largest] or [i for i in range(1, amount) if holding[i] < bound]
        pool, remaining = sum([portions[i] for i in free]), surplus
        for i in free:
            extra = min(bound - holding[i], max(1, remaining * portions[i] // pool), surplus)
            holding[i] = holding[i] + extra
            surplus = surplus - extra
    return np.array(holding)


def noise(stream_key, shape, deviation, reach, cuts=(), kind=jnp.bfloat16):
    factor_of = levels(stream_key, shape, cuts, -0.22, 0.18) if cuts else 1.0
    result = jax.random.normal(stream_key, shape, jnp.float32) * deviation * factor_of
    return jnp.minimum(jnp.maximum(result, -reach), reach).astype(kind)


def setup_inputs(seed: int = 0, part: int = 0) -> dict:
    streams_of = jax.random.split(jax.random.key(seed), 7)
    part_splits = jax.random.split(jax.random.fold_in(streams_of[6], part), 7)
    tokens = noise(part_splits[0], (TOKENS, D), 1.0, 6.0, ((0, 32),))
    route_ids_keys = jax.random.split(jax.random.fold_in(part_splits[1], 1), TOKENS // TOK_DEV)
    route_ids_turns = jax.random.permutation(jax.random.fold_in(part_splits[1], 3), TOKENS // TOK_DEV)
    route_ids = jax.vmap(lambda own, number: deal_out(jax.random.fold_in(part_splits[1], 2), own, number, TOK_DEV, EXPERTS, TOP, CAP, 2))(route_ids_keys, route_ids_turns).reshape((TOKENS, TOP))
    route_gates = jnp.clip(jnp.exp(math.log(1.0) - 2.3025851 * jax.random.uniform(part_splits[2], (TOKENS, TOP), jnp.float32) ** levels(part_splits[2], (TOKENS, TOP), ((0, 32),), -0.2, 0.2)), 0.1, 1.0)
    gate_weight = noise(streams_of[3], (D, EXPERTS * FF), D ** -0.5, 0.09375, ((1, 256),))
    up_weight = noise(streams_of[4], (D, EXPERTS * FF), D ** -0.5, 0.09375, ((1, 256),))
    down_weight = noise(streams_of[5], (EXPERTS * FF, D), FF ** -0.5, 0.0625, ((0, 32), (1, 8)))
    return {"tokens": tokens, "route_ids": route_ids, "route_gates": route_gates, "gate_weight": gate_weight, "up_weight": up_weight, "down_weight": down_weight}


def reference(tokens, route_ids, route_gates, gate_weight, up_weight, down_weight):
    floats = tokens.astype(jnp.float32)
    scale = lax.rsqrt(lax.optimization_barrier(jnp.mean(floats * floats, axis=-1, keepdims=True)) + 1e-05)
    normed = (floats * scale).astype(jnp.bfloat16)

    def per_expert(total, expert):
        start = expert * FF
        gate_cols = lax.dynamic_slice_in_dim(gate_weight, start, FF, 1)
        up_cols = lax.dynamic_slice_in_dim(up_weight, start, FF, 1)
        down_rows = lax.dynamic_slice_in_dim(down_weight, start, FF, 0)
        gate_sum = jnp.dot(normed, gate_cols, preferred_element_type=jnp.float32)
        up_sum = jnp.dot(normed, up_cols, preferred_element_type=jnp.float32)
        hidden = (jax.nn.silu(gate_sum) * up_sum).astype(jnp.bfloat16)
        produced = jnp.dot(hidden, down_rows, preferred_element_type=jnp.float32)
        weight = lax.optimization_barrier(jnp.sum(jnp.where(route_ids == expert, route_gates, 0.0), axis=1))
        return (total + produced * weight[:, None], None)
    mixture, unused = lax.scan(per_expert, jnp.zeros((TOKENS, D), jnp.float32), jnp.arange(EXPERTS, dtype=jnp.int32))
    return (floats + mixture).astype(jnp.bfloat16)
```

```python
import jax
import jax.numpy as jnp
from jax import lax
from jax.sharding import Mesh, PartitionSpec as P

EXPERTS = 4
TOP = 2
CAP = 24
NEAR = 4
CORES = 2

EPSILON = 1e-05


def slot_index(id_table):
    flat_ids = id_table.reshape(-1)
    onehot = (flat_ids[:, None] == jnp.arange(EXPERTS, dtype=jnp.int32)[None, :]).astype(jnp.int32)
    earlier = jnp.cumsum(onehot, axis=0) - onehot
    position = jnp.sum(earlier * onehot, axis=1)
    return (flat_ids * CAP + position).reshape(id_table.shape)


def from_everyone(array, axis):
    devices = lax.axis_size(axis)
    return lax.all_to_all(
        jnp.broadcast_to(array[None], (devices, *array.shape)), axis, 0, 0, tiled=True
    )


def local(tokens, route_ids, route_gates, gate_weight, up_weight, down_weight):
    f32, bf16 = jnp.float32, jnp.bfloat16
    tok_count, model_width = tokens.shape
    far, near, xs = lax.axis_size("far"), lax.axis_size("near"), lax.axis_size("x")
    core, x = lax.axis_index("core"), lax.axis_index("x")
    part = CAP // CORES
    chip_width = model_width // xs
    out_width = down_weight.shape[1]
    swap = [(i, (i + 1) % CORES) for i in range(CORES)]
    gate_other = lax.ppermute(gate_weight, "core", swap)
    up_other = lax.ppermute(up_weight, "core", swap)
    down_other = lax.ppermute(down_weight, "core", swap)

    floats = tokens.astype(f32)
    scale = lax.rsqrt(jnp.mean(floats * floats, axis=-1, keepdims=True) + EPSILON)
    chip_cols = lax.dynamic_slice_in_dim(tokens, x * chip_width, chip_width, 1)
    normed = (chip_cols.astype(f32) * scale).astype(bf16)

    slot_of = slot_index(route_ids)
    targets = (
        jnp.arange(EXPERTS, dtype=jnp.int32)[:, None] * CAP
        + core * part
        + jnp.arange(part, dtype=jnp.int32)[None, :]
    ).reshape(-1)
    matches = slot_of[:, :, None] == targets[None, None, :]
    combine = jnp.sum(jnp.where(matches, route_gates[:, :, None], 0.0), axis=1)
    picker = jnp.sum(matches.astype(f32), axis=1).astype(bf16)
    packed = jnp.dot(picker.T, normed, preferred_element_type=f32).astype(bf16)
    lanes = chip_width // 128
    packed = packed.reshape(EXPERTS, 1, part, lanes, 128)
    copies = far // EXPERTS
    sent = jnp.broadcast_to(packed, (EXPERTS, copies, part, lanes, 128))
    sent = sent.reshape(far, part, lanes, 128)
    arrived = lax.all_to_all(sent, "far", 0, 0, tiled=True)
    arrived = arrived.reshape(far * part, chip_width)
    rows = lax.all_gather(arrived, "near", axis=0, tiled=True)
    n_rows = rows.shape[0]
    full = from_everyone(rows, "x").reshape(xs, n_rows, chip_width)

    def project(weight):
        return jnp.einsum(
            "xsd,xdn->sn",
            full,
            weight.reshape(xs, chip_width, weight.shape[1]),
            preferred_element_type=f32,
        )

    hidden_own = (jax.nn.silu(project(gate_weight)) * project(up_weight)).astype(bf16)
    hidden_other = (jax.nn.silu(project(gate_other)) * project(up_other)).astype(bf16)
    first = core == 0
    hidden = jnp.concatenate(
        [
            jnp.where(first, hidden_own, hidden_other),
            jnp.where(first, hidden_other, hidden_own),
        ],
        axis=1,
    )
    units = from_everyone(hidden, "x")

    def down(weight):
        return jnp.einsum(
            "xsu,xun->sn",
            units.reshape(xs, n_rows, hidden.shape[1]),
            weight.reshape(xs, hidden.shape[1], out_width),
            preferred_element_type=f32,
        ).astype(bf16)

    produced = jnp.concatenate([down(down_weight), down(down_other)], axis=1)
    parts = lax.all_to_all(
        produced.reshape(near, far * part, 2 * out_width), "near", 0, 0, tiled=True
    )
    summed = jnp.sum(parts.astype(f32), axis=0).astype(bf16)
    out_lanes = 2 * out_width // 128
    returned = lax.all_to_all(
        summed.reshape(far, part, out_lanes, 128), "far", 0, 0, tiled=True
    )
    returned = jnp.sum(
        returned.reshape(EXPERTS, copies, part, out_lanes, 128).astype(f32), axis=1
    ).reshape(EXPERTS * part, 2 * out_width)
    mixture = jnp.dot(
        combine, returned, precision=lax.Precision.HIGHEST, preferred_element_type=f32
    )
    mixture = mixture[:, :out_width] + lax.ppermute(mixture[:, out_width:], "core", swap)
    residual = lax.dynamic_slice_in_dim(
        tokens, (x * CORES + core) * out_width, out_width, 1
    ).astype(f32)
    return (residual + mixture).astype(bf16)


def solution(mesh):
    groups, experts, tensor = (mesh.shape[n] for n in ("groups", "expert", "tensor"))
    fine = Mesh(
        mesh.devices.reshape(groups, experts // NEAR, NEAR, tensor // CORES, CORES),
        ("groups", "far", "near", "x", "core"),
    )
    tok = ("groups", "far", "near")
    in_specs = (
        P(tok, None),
        P(tok, None),
        P(tok, None),
        P(None, ("far", "near", "x", "core")),
        P(None, ("far", "near", "x", "core")),
        P(("far", "near"), ("x", "core")),
    )
    out_specs = P(tok, ("x", "core"))
    return jax.shard_map(local, mesh=fine, in_specs=in_specs, out_specs=out_specs, check_vma=False)
```

```python
import jax
import jax.numpy as jnp
from jax import lax
from jax.experimental import pallas as pl
from jax.sharding import Mesh, PartitionSpec as P


EXPERTS = 4
CAP = 24
NEAR = 4
CORES = 2

EPSILON = 1e-05


def slot_index(id_table):
    flat_ids = id_table.reshape(-1)
    onehot = (flat_ids[:, None] == jnp.arange(EXPERTS, dtype=jnp.int32)[None, :]).astype(jnp.int32)
    earlier = jnp.cumsum(onehot, axis=0) - onehot
    position = jnp.sum(earlier * onehot, axis=1)
    return (flat_ids * CAP + position).reshape(id_table.shape)


def from_everyone(array, axis):
    devices = lax.axis_size(axis)
    return lax.all_to_all(
        jnp.broadcast_to(array[None], (devices, *array.shape)), axis, 0, 0, tiled=True
    )


def product_kernel(rows, own, other, out):
    both = jnp.concatenate([own[0, 0], other[0, 0]], axis=1)
    product = jnp.dot(rows[...], both, preferred_element_type=jnp.float32)
    width = own.shape[-1]
    out[0, 0] = product[:, :width].astype(out.dtype)
    out[1, 0] = product[:, width:].astype(out.dtype)


def products(rows, own, other, shift, dtype):
    n_rows, depth = rows.shape
    kinds, width = own.shape[1], own.shape[3]
    weight_spec = pl.BlockSpec((1, 1, depth, width), lambda kind: (shift, kind, 0, 0))
    return pl.pallas_call(
        product_kernel,
        grid=(kinds,),
        in_specs=[pl.BlockSpec((n_rows, depth), lambda kind: (0, 0)), weight_spec, weight_spec],
        out_specs=pl.BlockSpec((CORES, 1, n_rows, width), lambda kind: (0, kind, 0, 0)),
        out_shape=jax.ShapeDtypeStruct((CORES, kinds, n_rows, width), dtype),
        cost_estimate=pl.CostEstimate(
            flops=2 * n_rows * depth * width * kinds * CORES,
            bytes_accessed=2 * depth * width * kinds * CORES,
            transcendentals=0,
        ),
    )(rows, own, other)


def layer(tokens, route_ids, route_gates, gate_weight, up_weight, down_weight):
    f32, bf16 = jnp.float32, jnp.bfloat16
    _, model_width = tokens.shape
    far, near, xs = lax.axis_size("far"), lax.axis_size("near"), lax.axis_size("x")
    core, x = lax.axis_index("core"), lax.axis_index("x")
    part = CAP // CORES
    chip_width = model_width // xs
    out_width = down_weight.shape[1]
    swap = [(i, (i + 1) % CORES) for i in range(CORES)]

    def chunk(shift):
        start = (x + shift) % xs * chip_width
        return jnp.stack(
            [
                lax.dynamic_slice_in_dim(weight, start, chip_width, 0)
                for weight in (gate_weight, up_weight)
            ]
        )

    chunks = [chunk(0)]
    for shift in range(1, xs):
        chunks.append(lax.ppermute(chunk(shift), "x", [(i, (i + shift) % xs) for i in range(xs)]))
    own = jnp.stack(chunks)
    down_other = lax.ppermute(down_weight, "core", swap)

    floats = tokens.astype(f32)
    scale = lax.rsqrt(jnp.mean(floats * floats, axis=-1, keepdims=True) + EPSILON)
    chip_cols = lax.dynamic_slice_in_dim(tokens, x * chip_width, chip_width, 1)
    normed = (chip_cols.astype(f32) * scale).astype(bf16)

    slot_of = slot_index(route_ids)
    targets = (
        jnp.arange(EXPERTS, dtype=jnp.int32)[:, None] * CAP
        + core * part
        + jnp.arange(part, dtype=jnp.int32)[None, :]
    ).reshape(-1)
    matches = slot_of[:, :, None] == targets[None, None, :]
    combine = jnp.sum(jnp.where(matches, route_gates[:, :, None], 0.0), axis=1)
    picker = jnp.sum(matches.astype(f32), axis=1).astype(bf16)
    packed = jnp.dot(picker.T, normed, preferred_element_type=f32).astype(bf16)
    lanes = chip_width // 128
    packed = packed.reshape(EXPERTS, 1, part, lanes, 128)
    copies = far // EXPERTS
    sent = jnp.broadcast_to(packed, (EXPERTS, copies, part, lanes, 128))
    sent = sent.reshape(far, part, lanes, 128)
    arrived = lax.all_to_all(sent, "far", 0, 0, tiled=True)
    arrived, own = lax.optimization_barrier((arrived.reshape(far * part, chip_width), own))
    other = lax.ppermute(own, "core", swap)
    rows = lax.all_gather(arrived, "near", axis=0, tiled=True)
    n_rows = rows.shape[0]

    total = products(rows, own, other, 0, f32)
    for shift in range(1, xs):
        total = total + lax.ppermute(
            products(rows, own, other, shift, bf16),
            "x",
            [(i, (i - shift) % xs) for i in range(xs)],
        ).astype(f32)
    hidden_own, hidden_other = (jax.nn.silu(total[:, 0]) * total[:, 1]).astype(bf16)
    first = core == 0
    hidden = jnp.concatenate(
        [
            jnp.where(first, hidden_own, hidden_other),
            jnp.where(first, hidden_other, hidden_own),
        ],
        axis=1,
    )
    units = from_everyone(hidden, "x")

    def down(weight):
        return jnp.einsum(
            "xsu,xun->sn",
            units.reshape(xs, n_rows, hidden.shape[1]),
            weight.reshape(xs, hidden.shape[1], out_width),
            preferred_element_type=f32,
        ).astype(bf16)

    produced = jnp.concatenate([down(down_weight), down(down_other)], axis=1)
    parts = lax.all_to_all(
        produced.reshape(near, far * part, 2 * out_width), "near", 0, 0, tiled=True
    )
    summed = jnp.sum(parts.astype(f32), axis=0).astype(bf16)
    out_lanes = 2 * out_width // 128
    returned = lax.all_to_all(
        summed.reshape(far, part, out_lanes, 128), "far", 0, 0, tiled=True
    )
    returned = jnp.sum(
        returned.reshape(EXPERTS, copies, part, out_lanes, 128).astype(f32), axis=1
    ).reshape(EXPERTS * part, 2 * out_width)
    mixture = jnp.dot(
        combine, returned, precision=lax.Precision.HIGHEST, preferred_element_type=f32
    )
    mixture = mixture[:, :out_width] + lax.ppermute(mixture[:, out_width:], "core", swap)
    residual = lax.dynamic_slice_in_dim(
        tokens, (x * CORES + core) * out_width, out_width, 1
    ).astype(f32)
    return (residual + mixture).astype(bf16)


def solution(mesh):
    groups, experts, tensor = (mesh.shape[n] for n in ("groups", "expert", "tensor"))
    fine = Mesh(
        mesh.devices.reshape(groups, experts // NEAR, NEAR, tensor // CORES, CORES),
        ("groups", "far", "near", "x", "core"),
    )
    tok = ("groups", "far", "near")
    in_specs = (
        P(tok, None),
        P(tok, None),
        P(tok, None),
        P(None, ("far", "near", "x", "core")),
        P(None, ("far", "near", "x", "core")),
        P(("far", "near"), ("x", "core")),
    )
    out_specs = P(tok, ("x", "core"))
    return jax.shard_map(layer, mesh=fine, in_specs=in_specs, out_specs=out_specs, check_vma=False)
```

```python
import jax
import jax.numpy as jnp
from jax import lax
from jax.experimental import pallas as pl
from jax.experimental.pallas import tpu as pltpu
from jax.sharding import Mesh, PartitionSpec as P


EXPERTS = 4
CAP = 24
NEAR = 4
CORES = 2
PART = CAP // CORES
SLOTS = EXPERTS * PART

EPSILON = 1e-05


def pack_kernel(place, tokens, ids, gates, packed, combine):
    f32, bf16 = jnp.float32, jnp.bfloat16
    width = packed.shape[1]
    rows = tokens.shape[0]
    floats = tokens[...].astype(f32)
    scale = lax.rsqrt(jnp.mean(floats * floats, axis=1, keepdims=True) + EPSILON)
    start = pl.multiple_of(place[0] * width, width)
    normed = (tokens[:, pl.ds(start, width)].astype(f32) * scale).astype(bf16)
    slot = lax.broadcasted_iota(jnp.int32, (SLOTS, rows), 0)
    expert = sum((slot >= PART * e).astype(jnp.int32) for e in range(1, EXPERTS))
    wanted = (slot - expert * PART + place[1] * PART).astype(f32)
    first = ids[0:1, :] == expert
    second = ids[1:2, :] == expert
    named = jnp.where(jnp.logical_or(first, second), 1.0, 0.0)
    before = jnp.where(
        lax.broadcasted_iota(jnp.int32, (rows, rows), 0)
        < lax.broadcasted_iota(jnp.int32, (rows, rows), 1),
        1.0,
        0.0,
    ).astype(bf16)
    position = jnp.dot(named.astype(bf16), before, preferred_element_type=f32)
    picker = jnp.where(position == wanted, named, 0.0)
    gate = jnp.where(first, gates[0:1, :], jnp.where(second, gates[1:2, :], 0.0))
    combine[...] = picker * gate
    packed[...] = jnp.dot(picker.astype(bf16), normed, preferred_element_type=f32).astype(bf16)


def pack(place, tokens, ids, gates, width):
    rows = tokens.shape[0]
    whole = pl.BlockSpec(memory_space=pltpu.VMEM)
    return pl.pallas_call(
        pack_kernel,
        in_specs=[pl.BlockSpec(memory_space=pltpu.SMEM), whole, whole, whole],
        out_specs=[whole, whole],
        out_shape=[
            jax.ShapeDtypeStruct((SLOTS, width), jnp.bfloat16),
            jax.ShapeDtypeStruct((SLOTS, rows), jnp.float32),
        ],
    )(place, tokens, ids.T, gates.T)


def product_kernel(place, rows, own, other, out):
    width = own.shape[-1]
    both = jnp.concatenate([own[0, 0], own[0, 1], other[0, 0], other[0, 1]], axis=1)
    product = jnp.dot(rows[...], both, preferred_element_type=jnp.float32).astype(out.dtype)
    for core in range(CORES):
        for kind in range(2):
            at = (core * 2 + kind) * width
            out[0, core, kind] = product[:, at : at + width]


def products(place, rows, own, other):
    n_rows, depth = rows.shape
    xs, kinds, width = own.shape[0], own.shape[1], own.shape[3]
    weight_spec = pl.BlockSpec((1, kinds, depth, width), lambda shift, place: (shift, 0, 0, 0))
    return pl.pallas_call(
        product_kernel,
        grid_spec=pltpu.PrefetchScalarGridSpec(
            num_scalar_prefetch=1,
            grid=(xs,),
            in_specs=[
                pl.BlockSpec((n_rows, depth), lambda shift, place: (0, 0)),
                weight_spec,
                weight_spec,
            ],
            out_specs=pl.BlockSpec(
                (1, CORES, kinds, n_rows, width),
                lambda shift, place: (lax.rem(place[0] + xs - shift, xs), 0, 0, 0, 0),
            ),
        ),
        out_shape=jax.ShapeDtypeStruct((xs, CORES, kinds, n_rows, width), jnp.bfloat16),
    )(place, rows, own, other)


def hidden_kernel(place, sums, out):
    f32 = jnp.float32
    total = jnp.sum(sums[...].astype(f32), axis=0)
    width = sums.shape[-1]
    gate, up = total[:, 0], total[:, 1]
    hidden = (gate / (1.0 + jnp.exp(-gate)) * up).astype(out.dtype)
    straight = place[1] == 0
    low = jnp.where(straight, hidden[0], hidden[1])
    high = jnp.where(straight, hidden[1], hidden[0])
    for copy in range(out.shape[0]):
        out[copy, :, 0:width] = low
        out[copy, :, width : 2 * width] = high


def hidden_units(place, sums):
    xs, cores, kinds, n_rows, width = sums.shape
    block = n_rows // 3
    return pl.pallas_call(
        hidden_kernel,
        grid_spec=pltpu.PrefetchScalarGridSpec(
            num_scalar_prefetch=1,
            grid=(n_rows // block,),
            in_specs=[
                pl.BlockSpec((xs, cores, kinds, block, width), lambda i, place: (0, 0, 0, i, 0))
            ],
            out_specs=pl.BlockSpec((xs, block, cores * width), lambda i, place: (0, i, 0)),
        ),
        out_shape=jax.ShapeDtypeStruct((xs, n_rows, cores * width), jnp.bfloat16),
    )(place, sums)


def layer(tokens, route_ids, route_gates, gate_weight, up_weight, down_weight):
    f32, bf16 = jnp.float32, jnp.bfloat16
    model_width = tokens.shape[1]
    far, near, xs = lax.axis_size("far"), lax.axis_size("near"), lax.axis_size("x")
    core, x = lax.axis_index("core"), lax.axis_index("x")
    chip_width = model_width // xs
    out_width = down_weight.shape[1]
    lanes = chip_width // 128
    copies = far // EXPERTS
    swap = [(i, (i + 1) % CORES) for i in range(CORES)]
    place = jnp.stack([x, core]).astype(jnp.int32)

    packed, combine = pack(place, tokens, route_ids, route_gates, chip_width)
    sent = jnp.broadcast_to(
        packed.reshape(EXPERTS, 1, PART, lanes, 128), (EXPERTS, copies, PART, lanes, 128)
    ).reshape(far, PART, lanes, 128)
    arrived = lax.all_to_all(sent, "far", 0, 0, tiled=True)

    def chunk(shift):
        start = (x + shift) % xs * chip_width
        return jnp.stack(
            [
                lax.dynamic_slice_in_dim(weight, start, chip_width, 0)
                for weight in (gate_weight, up_weight)
            ]
        )

    chunks = [chunk(0)]
    for shift in range(1, xs):
        chunks.append(lax.ppermute(chunk(shift), "x", [(i, (i + shift) % xs) for i in range(xs)]))
    own = jnp.stack(chunks)
    other = lax.ppermute(own, "core", swap)
    down_other = lax.ppermute(down_weight, "core", swap)

    arrived = arrived.reshape(1, far * PART, chip_width)
    rows = lax.all_to_all(
        jnp.broadcast_to(arrived, (near, far * PART, chip_width)), "near", 0, 0, tiled=True
    )
    n_rows = near * far * PART
    partial = products(place, rows.reshape(n_rows, chip_width), own, other)
    sums = lax.all_to_all(partial, "x", 0, 0, tiled=True)
    units = lax.all_to_all(hidden_units(place, sums), "x", 0, 0, tiled=True)

    def down(weight):
        return jnp.einsum(
            "xsu,xun->sn",
            units,
            weight.reshape(xs, units.shape[2], out_width),
            preferred_element_type=f32,
        ).astype(bf16)

    produced = jnp.concatenate([down(down_weight), down(down_other)], axis=1)
    parts = lax.all_to_all(
        produced.reshape(near, far * PART, 2 * out_width), "near", 0, 0, tiled=True
    )
    summed = jnp.sum(parts.astype(f32), axis=0).astype(bf16)
    out_lanes = 2 * out_width // 128
    returned = lax.all_to_all(
        summed.reshape(far, PART, out_lanes, 128), "far", 0, 0, tiled=True
    )
    returned = jnp.sum(
        returned.reshape(EXPERTS, copies, PART, out_lanes, 128).astype(f32), axis=1
    ).reshape(SLOTS, 2 * out_width)
    mixture = jnp.einsum(
        "st,sd->td",
        combine,
        returned,
        precision=lax.Precision.HIGHEST,
        preferred_element_type=f32,
    )
    mixture = mixture[:, :out_width] + lax.ppermute(mixture[:, out_width:], "core", swap)
    residual = lax.dynamic_slice_in_dim(
        tokens, (x * CORES + core) * out_width, out_width, 1
    ).astype(f32)
    return (residual + mixture).astype(bf16)


def solution(mesh):
    groups, experts, tensor = (mesh.shape[n] for n in ("groups", "expert", "tensor"))
    fine = Mesh(
        mesh.devices.reshape(groups, experts // NEAR, NEAR, tensor // CORES, CORES),
        ("groups", "far", "near", "x", "core"),
    )
    tok = ("groups", "far", "near")
    in_specs = (
        P(tok, None),
        P(tok, None),
        P(tok, None),
        P(None, ("far", "near", "x", "core")),
        P(None, ("far", "near", "x", "core")),
        P(("far", "near"), ("x", "core")),
    )
    out_specs = P(tok, ("x", "core"))
    return jax.shard_map(layer, mesh=fine, in_specs=in_specs, out_specs=out_specs, check_vma=False)
```

```python
import jax
import jax.numpy as jnp
from jax import lax
from jax.experimental import pallas as pl
from jax.experimental.pallas import tpu as pltpu
from jax.sharding import Mesh, PartitionSpec as P


EXPERTS = 4
CAP = 24
NEAR = 4
CORES = 2
PART = CAP // CORES
SLOTS = EXPERTS * PART

EPSILON = 1e-05


def whole(space=None):
    return pl.BlockSpec(memory_space=space or pltpu.VMEM)


PARAMS = pltpu.CompilerParams(vmem_limit_bytes=16 << 20)


def near_memory(*arrays):
    return [pltpu.with_memory_space_constraint(array, pltpu.VMEM) for array in arrays]


def pack_kernel(tokens, ids, gates, packed, combine, residual):
    f32, bf16 = jnp.float32, jnp.bfloat16
    half = packed.shape[2]
    rows = tokens.shape[0]
    x, core = lax.axis_index("x"), lax.axis_index("core")
    out_width = residual.shape[1]
    floats = tokens[...].astype(f32)
    scale = lax.rsqrt(jnp.mean(floats * floats, axis=1, keepdims=True) + EPSILON)
    slot = lax.broadcasted_iota(jnp.int32, (SLOTS, rows), 0)
    expert = sum((slot >= PART * e).astype(jnp.int32) for e in range(1, EXPERTS))
    wanted = (slot - expert * PART + core * PART).astype(f32)
    first = ids[0:1, :] == expert
    second = ids[1:2, :] == expert
    before = jnp.where(
        lax.broadcasted_iota(jnp.int32, (rows, rows), 0)
        < lax.broadcasted_iota(jnp.int32, (rows, rows), 1),
        1.0,
        0.0,
    ).astype(bf16)

    def picked(named, wanted):
        position = jnp.dot(named.astype(bf16), before, preferred_element_type=f32)
        return jnp.where(position == wanted, named, 0.0)

    gate = jnp.where(first, gates[0:1, :], jnp.where(second, gates[1:2, :], 0.0))
    named = jnp.where(jnp.logical_or(first, second), 1.0, 0.0)
    combine[...] = picked(named, wanted) * gate
    line = lax.broadcasted_iota(jnp.int32, (2 * SLOTS, rows), 0)
    expert = sum((line >= 2 * PART * e).astype(jnp.int32) for e in range(1, EXPERTS))
    at = line - expert * (2 * PART)
    upper = (at >= PART).astype(jnp.int32)
    wanted = (at - upper * PART + core * PART).astype(f32)
    named = jnp.where(jnp.logical_or(ids[0:1, :] == expert, ids[1:2, :] == expert), 1.0, 0.0)
    picker = picked(named, wanted)
    total = jnp.zeros((2 * SLOTS, half), f32)
    for part in range(2):
        start = pl.multiple_of((x * 2 + part) * half, half)
        normed = (tokens[:, pl.ds(start, half)].astype(f32) * scale).astype(bf16)
        mine = jnp.where(upper == part, picker, 0.0).astype(bf16)
        total = total + jnp.dot(mine, normed, preferred_element_type=f32)
    total = total.astype(bf16)
    copies = packed.shape[0] // EXPERTS
    for e in range(EXPERTS):
        for copy in range(copies):
            packed[e * copies + copy] = total[e * 2 * PART : (e + 1) * 2 * PART]
    start = pl.multiple_of((x * CORES + core) * out_width, out_width)
    residual[...] = tokens[:, pl.ds(start, out_width)]


def pack(tokens, ids, gates, far, chip_width, out_width):
    rows = tokens.shape[0]
    return pl.pallas_call(
        pack_kernel,
        compiler_params=PARAMS,
        in_specs=[whole()] * 3,
        out_specs=[whole()] * 3,
        out_shape=[
            pltpu.VMEM((far, 2 * PART, chip_width // 2), jnp.bfloat16),
            pltpu.VMEM((SLOTS, rows), jnp.float32),
            pltpu.VMEM((rows, out_width), jnp.bfloat16),
        ],
    )(tokens, ids.T, gates.T)


def product_kernel(rows, own, other, out):
    xs, kinds, _, width = own.shape
    x = lax.axis_index("x")
    left = rows[...]
    for shift in range(xs):
        to = lax.rem(x + (xs - shift), xs)
        for core, weights in enumerate((own, other)):
            both = jnp.concatenate([weights[shift, kind] for kind in range(kinds)], axis=1)
            product = jnp.dot(left, both, preferred_element_type=jnp.float32).astype(out.dtype)
            for kind in range(kinds):
                out[to, core, kind] = product[:, kind * width : (kind + 1) * width]


def products(rows, own, other):
    n_rows = rows.shape[0]
    xs, kinds, _, width = own.shape
    return pl.pallas_call(
        product_kernel,
        compiler_params=PARAMS,
        in_specs=[whole()] * 3,
        out_specs=whole(),
        out_shape=pltpu.VMEM((xs, CORES, kinds, n_rows, width), jnp.bfloat16),
    )(*near_memory(rows, own, other))


def hidden_kernel(sums, out):
    f32 = jnp.float32
    xs, _, _, n_rows, width = sums.shape
    straight = lax.axis_index("core") == 0
    block = 32
    for at in range(0, n_rows, block):
        total = sums[0, :, :, at : at + block, :].astype(f32)
        for source in range(1, xs):
            total = total + sums[source, :, :, at : at + block, :].astype(f32)
        gate, up = total[:, 0], total[:, 1]
        hidden = (gate / (1.0 + jnp.exp(-gate)) * up).astype(out.dtype)
        low = jnp.where(straight, hidden[0], hidden[1])
        high = jnp.where(straight, hidden[1], hidden[0])
        for copy in range(out.shape[0]):
            out[copy, at : at + block, 0:width] = low
            out[copy, at : at + block, width : 2 * width] = high


def hidden_units(sums):
    xs, cores, _, n_rows, width = sums.shape
    return pl.pallas_call(
        hidden_kernel,
        compiler_params=PARAMS,
        in_specs=[whole()],
        out_specs=whole(),
        out_shape=pltpu.VMEM((xs, n_rows, cores * width), jnp.bfloat16),
    )(*near_memory(sums))


def down_kernel(units, own, other, out):
    xs, _, _ = units.shape
    near, block, _ = out.shape
    width = own.shape[1]
    left = jnp.concatenate([units[source] for source in range(xs)], axis=1)
    for core, weight in enumerate((own, other)):
        product = jnp.dot(left, weight[...], preferred_element_type=jnp.float32).astype(out.dtype)
        for line in range(near):
            out[line, :, core * width : (core + 1) * width] = product[
                line * block : (line + 1) * block
            ]


def down(units, own, other, near):
    n_rows = units.shape[1]
    return pl.pallas_call(
        down_kernel,
        compiler_params=PARAMS,
        in_specs=[whole()] * 3,
        out_specs=whole(),
        out_shape=pltpu.VMEM((near, n_rows // near, CORES * own.shape[1]), jnp.bfloat16),
    )(*near_memory(units, own, other))


def layer(tokens, route_ids, route_gates, gate_weight, up_weight, down_weight):
    f32, bf16 = jnp.float32, jnp.bfloat16
    model_width = tokens.shape[1]
    far, near, xs = lax.axis_size("far"), lax.axis_size("near"), lax.axis_size("x")
    x = lax.axis_index("x")
    chip_width = model_width // xs
    out_width = down_weight.shape[1]
    copies = far // EXPERTS
    swap = [(i, (i + 1) % CORES) for i in range(CORES)]
    sent, combine, residual = pack(tokens, route_ids, route_gates, far, chip_width, out_width)
    arrived = lax.all_to_all(sent, "far", 0, 0, tiled=True)

    def chunk(shift):
        start = (x + shift) % xs * chip_width
        return jnp.stack(
            [
                lax.dynamic_slice_in_dim(weight, start, chip_width, 0)
                for weight in (gate_weight, up_weight)
            ]
        )

    chunks = [chunk(0)]
    for shift in range(1, xs):
        chunks.append(lax.ppermute(chunk(shift), "x", [(i, (i + shift) % xs) for i in range(xs)]))
    own = jnp.stack(chunks)
    other = lax.ppermute(own, "core", swap)
    down_other = lax.ppermute(down_weight, "core", swap)

    arrived = arrived.reshape(far, 2, PART, chip_width // 2)
    arrived = jnp.swapaxes(arrived, 1, 2).reshape(1, far * PART, chip_width)
    rows = lax.all_to_all(
        jnp.broadcast_to(arrived, (near, far * PART, chip_width)), "near", 0, 0, tiled=True
    )
    n_rows = near * far * PART
    partial = products(rows.reshape(n_rows, chip_width), own, other)
    sums = lax.all_to_all(partial, "x", 0, 0, tiled=True)
    units = lax.all_to_all(hidden_units(sums), "x", 0, 0, tiled=True)
    produced = down(units, down_weight, down_other, near)
    parts = lax.all_to_all(produced, "near", 0, 0, tiled=True)
    summed = jnp.sum(parts.astype(f32), axis=0).astype(bf16)
    out_lanes = 2 * out_width // 128
    returned = lax.all_to_all(
        summed.reshape(far, PART, out_lanes, 128), "far", 0, 0, tiled=True
    )
    returned = jnp.sum(
        returned.reshape(EXPERTS, copies, PART, out_lanes, 128).astype(f32), axis=1
    ).reshape(SLOTS, 2 * out_width)
    mixture = jnp.einsum(
        "st,sd->td",
        combine,
        returned,
        precision=lax.Precision.HIGHEST,
        preferred_element_type=f32,
    )
    mixture = mixture[:, :out_width] + lax.ppermute(mixture[:, out_width:], "core", swap)
    return (residual.astype(f32) + mixture).astype(bf16)


def solution(mesh):
    groups, experts, tensor = (mesh.shape[n] for n in ("groups", "expert", "tensor"))
    fine = Mesh(
        mesh.devices.reshape(groups, experts // NEAR, NEAR, tensor // CORES, CORES),
        ("groups", "far", "near", "x", "core"),
    )
    tok = ("groups", "far", "near")
    in_specs = (
        P(tok, None),
        P(tok, None),
        P(tok, None),
        P(None, ("far", "near", "x", "core")),
        P(None, ("far", "near", "x", "core")),
        P(("far", "near"), ("x", "core")),
    )
    out_specs = P(tok, ("x", "core"))
    return jax.shard_map(layer, mesh=fine, in_specs=in_specs, out_specs=out_specs, check_vma=False)
```

```python
import jax
import jax.numpy as jnp
from jax import lax
from jax.experimental import pallas as pl
from jax.experimental.pallas import tpu as pltpu
from jax.sharding import Mesh, PartitionSpec as P


EXPERTS = 4
CAP = 24
NEAR = 4
CORES = 2
PART = CAP // CORES
SLOTS = EXPERTS * PART

EPSILON = 1e-05


def whole(space=None):
    return pl.BlockSpec(memory_space=space or pltpu.VMEM)


PARAMS = pltpu.CompilerParams(vmem_limit_bytes=16 << 20)


def near_memory(*arrays):
    return [pltpu.with_memory_space_constraint(array, pltpu.VMEM) for array in arrays]


def pack_kernel(*refs):
    sources, (packed, combine, residual), held, sems = refs[:3], refs[3:6], refs[6:9], refs[9]
    moves = [
        pltpu.make_async_copy(source, place, sems.at[number])
        for number, (source, place) in enumerate(zip(sources, held))
    ]
    for move in moves:
        move.start()
    for move in moves:
        move.wait()
    tokens, ids, gates = held
    f32, bf16 = jnp.float32, jnp.bfloat16
    half = packed.shape[2]
    rows = tokens.shape[0]
    x, core = lax.axis_index("x"), lax.axis_index("core")
    out_width = residual.shape[1]
    floats = tokens[...].astype(f32)
    scale = lax.rsqrt(jnp.mean(floats * floats, axis=1, keepdims=True) + EPSILON)
    slot = lax.broadcasted_iota(jnp.int32, (SLOTS, rows), 0)
    expert = sum((slot >= PART * e).astype(jnp.int32) for e in range(1, EXPERTS))
    wanted = (slot - expert * PART + core * PART).astype(f32)
    first = ids[0:1, :] == expert
    second = ids[1:2, :] == expert
    before = jnp.where(
        lax.broadcasted_iota(jnp.int32, (rows, rows), 0)
        < lax.broadcasted_iota(jnp.int32, (rows, rows), 1),
        1.0,
        0.0,
    ).astype(bf16)

    def picked(named, wanted):
        position = jnp.dot(named.astype(bf16), before, preferred_element_type=f32)
        return jnp.where(position == wanted, named, 0.0)

    gate = jnp.where(first, gates[0:1, :], jnp.where(second, gates[1:2, :], 0.0))
    named = jnp.where(jnp.logical_or(first, second), 1.0, 0.0)
    combine[...] = picked(named, wanted) * gate
    line = lax.broadcasted_iota(jnp.int32, (2 * SLOTS, rows), 0)
    expert = sum((line >= 2 * PART * e).astype(jnp.int32) for e in range(1, EXPERTS))
    at = line - expert * (2 * PART)
    upper = (at >= PART).astype(jnp.int32)
    wanted = (at - upper * PART + core * PART).astype(f32)
    named = jnp.where(jnp.logical_or(ids[0:1, :] == expert, ids[1:2, :] == expert), 1.0, 0.0)
    picker = picked(named, wanted)
    total = jnp.zeros((2 * SLOTS, half), f32)
    for part in range(2):
        start = pl.multiple_of((x * 2 + part) * half, half)
        normed = (tokens[:, pl.ds(start, half)].astype(f32) * scale).astype(bf16)
        mine = jnp.where(upper == part, picker, 0.0).astype(bf16)
        total = total + jnp.dot(mine, normed, preferred_element_type=f32)
    total = total.astype(bf16)
    copies = packed.shape[0] // EXPERTS
    for e in range(EXPERTS):
        for copy in range(copies):
            packed[e * copies + copy] = total[e * 2 * PART : (e + 1) * 2 * PART]
    start = pl.multiple_of((x * CORES + core) * out_width, out_width)
    residual[...] = tokens[:, pl.ds(start, out_width)]


def pack(tokens, ids, gates, far, chip_width, out_width):
    rows = tokens.shape[0]
    arrays = (tokens, ids.T, gates.T)
    return pl.pallas_call(
        pack_kernel,
        compiler_params=PARAMS,
        in_specs=[whole(pltpu.HBM)] * 3,
        out_specs=[whole()] * 3,
        out_shape=[
            pltpu.VMEM((far, 2 * PART, chip_width // 2), jnp.bfloat16),
            pltpu.VMEM((SLOTS, rows), jnp.float32),
            pltpu.VMEM((rows, out_width), jnp.bfloat16),
        ],
        scratch_shapes=[pltpu.VMEM(array.shape, array.dtype) for array in arrays]
        + [pltpu.SemaphoreType.DMA((3,))],
    )(*[pltpu.with_memory_space_constraint(array, pltpu.HBM) for array in arrays])


def own_kernel(rows, *refs):
    chunks, out, stacked, sems = refs[:-3], refs[-3], refs[-2], refs[-1]
    xs, width = len(chunks), out.shape[-1]
    moves = [
        pltpu.make_async_copy(weights, stacked.at[shift], sems.at[shift])
        for shift, weights in enumerate(chunks)
    ]
    for move in moves:
        move.start()
    x = lax.axis_index("x")
    left = rows[...]
    for shift, weights in enumerate(chunks):
        to = lax.rem(x + (xs - shift), xs)
        gate, up = weights[0], weights[1]
        product = jnp.dot(
            left, jnp.concatenate([gate, up], axis=1), preferred_element_type=jnp.float32
        ).astype(out.dtype)
        out[to, 0] = product[:, :width]
        out[to, 1] = product[:, width:]
    for move in moves:
        move.wait()


def own_products(rows, chunks):
    xs, n_rows = len(chunks), rows.shape[0]
    return pl.pallas_call(
        own_kernel,
        compiler_params=PARAMS,
        in_specs=[whole()] * (1 + xs),
        out_specs=[whole(), whole(pltpu.HBM)],
        out_shape=[
            pltpu.VMEM((xs, 2, n_rows, chunks[0].shape[2]), jnp.bfloat16),
            pltpu.HBM((xs, *chunks[0].shape), jnp.bfloat16),
        ],
        scratch_shapes=[pltpu.SemaphoreType.DMA((xs,))],
    )(rows, *chunks)


def other_kernel(rows, stacked, out):
    xs, _, _, width = stacked.shape
    x = lax.axis_index("x")
    left = rows[...]
    for shift in range(xs):
        to = lax.rem(x + (xs - shift), xs)
        both = jnp.concatenate([stacked[shift, 0], stacked[shift, 1]], axis=1)
        product = jnp.dot(left, both, preferred_element_type=jnp.float32).astype(out.dtype)
        out[to, 0] = product[:, :width]
        out[to, 1] = product[:, width:]


def other_products(rows, stacked):
    xs, _, _, width = stacked.shape
    return pl.pallas_call(
        other_kernel,
        compiler_params=PARAMS,
        in_specs=[whole()] * 2,
        out_specs=whole(),
        out_shape=pltpu.VMEM((xs, 2, rows.shape[0], width), jnp.bfloat16),
    )(rows, stacked)


def hidden_of(sums, at, block, dtype):
    f32 = jnp.float32
    total = sums[0, :, at : at + block, :].astype(f32)
    for source in range(1, sums.shape[0]):
        total = total + sums[source, :, at : at + block, :].astype(f32)
    gate, up = total[0], total[1]
    return (gate / (1.0 + jnp.exp(-gate)) * up).astype(dtype)


def first_kernel(sums, out):
    block = 64
    for at in range(0, out.shape[0], block):
        out[at : at + block, :] = hidden_of(sums, at, block, out.dtype)


def first_units(sums):
    return pl.pallas_call(
        first_kernel,
        compiler_params=PARAMS,
        in_specs=[whole()],
        out_specs=whole(),
        out_shape=pltpu.VMEM(sums.shape[2:], jnp.bfloat16),
    )(*near_memory(sums))


def hidden_kernel(ready, sums, out):
    straight = lax.axis_index("core") == 0
    block, width = 64, ready.shape[1]
    for at in range(0, ready.shape[0], block):
        mine = ready[at : at + block, :]
        theirs = hidden_of(sums, at, block, out.dtype)
        low = jnp.where(straight, mine, theirs)
        high = jnp.where(straight, theirs, mine)
        for copy in range(out.shape[0]):
            out[copy, at : at + block, 0:width] = low
            out[copy, at : at + block, width : 2 * width] = high


def hidden_units(ready, sums):
    xs, _, n_rows, width = sums.shape
    return pl.pallas_call(
        hidden_kernel,
        compiler_params=PARAMS,
        in_specs=[whole()] * 2,
        out_specs=whole(),
        out_shape=pltpu.VMEM((xs, n_rows, CORES * width), jnp.bfloat16),
    )(*near_memory(ready, sums))


def down_kernel(units, own, other, out):
    xs, _, _ = units.shape
    near, block, _ = out.shape
    width = own.shape[1]
    left = jnp.concatenate([units[source] for source in range(xs)], axis=1)
    for core, weight in enumerate((own, other)):
        product = jnp.dot(left, weight[...], preferred_element_type=jnp.float32).astype(out.dtype)
        for line in range(near):
            out[line, :, core * width : (core + 1) * width] = product[
                line * block : (line + 1) * block
            ]


def down(units, own, other, near):
    n_rows = units.shape[1]
    return pl.pallas_call(
        down_kernel,
        compiler_params=PARAMS,
        in_specs=[whole()] * 3,
        out_specs=whole(),
        out_shape=pltpu.VMEM((near, n_rows // near, CORES * own.shape[1]), jnp.bfloat16),
    )(*near_memory(units, own, other))


def layer(tokens, route_ids, route_gates, gate_weight, up_weight, down_weight):
    f32, bf16 = jnp.float32, jnp.bfloat16
    model_width = tokens.shape[1]
    far, near, xs = lax.axis_size("far"), lax.axis_size("near"), lax.axis_size("x")
    x = lax.axis_index("x")
    chip_width = model_width // xs
    out_width = down_weight.shape[1]
    copies = far // EXPERTS
    swap = [(i, (i + 1) % CORES) for i in range(CORES)]
    sent, combine, residual = pack(tokens, route_ids, route_gates, far, chip_width, out_width)
    arrived = lax.all_to_all(sent, "far", 0, 0, tiled=True)

    def chunk(shift):
        start = (x + shift) % xs * chip_width
        return jnp.stack(
            [
                lax.dynamic_slice_in_dim(weight, start, chip_width, 0)
                for weight in (gate_weight, up_weight)
            ]
        )

    chunks = [chunk(0)]
    for shift in range(1, xs):
        chunks.append(lax.ppermute(chunk(shift), "x", [(i, (i + shift) % xs) for i in range(xs)]))
    down_other = lax.ppermute(down_weight, "core", swap)

    arrived = arrived.reshape(far, 2, PART, chip_width // 2)
    arrived = jnp.swapaxes(arrived, 1, 2).reshape(far * PART, chip_width)
    rows = lax.all_gather(arrived, "near", axis=0, tiled=True)
    mine, stacked = own_products(rows, chunks)
    mine = lax.all_to_all(mine, "x", 0, 0, tiled=True)
    stacked = lax.ppermute(stacked, "core", swap)
    theirs = other_products(rows, stacked)
    theirs = lax.all_to_all(theirs, "x", 0, 0, tiled=True)
    ready = first_units(mine)
    units = lax.all_to_all(hidden_units(ready, theirs), "x", 0, 0, tiled=True)
    produced = down(units, down_weight, down_other, near)
    parts = lax.all_to_all(produced, "near", 0, 0, tiled=True)
    summed = jnp.sum(parts.astype(f32), axis=0).astype(bf16)
    out_lanes = 2 * out_width // 128
    returned = lax.all_to_all(
        summed.reshape(far, PART, out_lanes, 128), "far", 0, 0, tiled=True
    )
    returned = jnp.sum(
        returned.reshape(EXPERTS, copies, PART, out_lanes, 128).astype(f32), axis=1
    ).reshape(SLOTS, 2 * out_width)
    mixture = jnp.einsum(
        "st,sd->td",
        combine,
        returned,
        precision=lax.Precision.HIGHEST,
        preferred_element_type=f32,
    )
    mixture = mixture[:, :out_width] + lax.ppermute(mixture[:, out_width:], "core", swap)
    return (residual.astype(f32) + mixture).astype(bf16)


def solution(mesh):
    groups, experts, tensor = (mesh.shape[n] for n in ("groups", "expert", "tensor"))
    fine = Mesh(
        mesh.devices.reshape(groups, experts // NEAR, NEAR, tensor // CORES, CORES),
        ("groups", "far", "near", "x", "core"),
    )
    tok = ("groups", "far", "near")
    in_specs = (
        P(tok, None),
        P(tok, None),
        P(tok, None),
        P(None, ("far", "near", "x", "core")),
        P(None, ("far", "near", "x", "core")),
        P(("far", "near"), ("x", "core")),
    )
    out_specs = P(tok, ("x", "core"))
    return jax.shard_map(layer, mesh=fine, in_specs=in_specs, out_specs=out_specs, check_vma=False)
```

```python
import jax
import jax.numpy as jnp
from jax import lax
from jax.experimental import pallas as pl
from jax.experimental.pallas import tpu as pltpu
from jax.sharding import Mesh, PartitionSpec as P


EXPERTS = 4
CAP = 24
NEAR = 4
CORES = 2
PART = CAP // CORES

EPSILON = 1e-05


def whole(space=None):
    return pl.BlockSpec(memory_space=space or pltpu.VMEM)


PARAMS = pltpu.CompilerParams(vmem_limit_bytes=16 << 20)


def near_memory(*arrays):
    return [pltpu.with_memory_space_constraint(array, pltpu.VMEM) for array in arrays]


def pack_kernel(*refs):
    sources, (packed, combine, residual), held, sems = refs[:3], refs[3:6], refs[6:9], refs[9]
    moves = [
        pltpu.make_async_copy(source, place, sems.at[number])
        for number, (source, place) in enumerate(zip(sources, held))
    ]
    for move in moves:
        move.start()
    for move in moves:
        move.wait()
    tokens, ids, gates = held
    f32, bf16 = jnp.float32, jnp.bfloat16
    width = packed.shape[2]
    rows = tokens.shape[0]
    slots = EXPERTS * CAP
    floats = tokens[...].astype(f32)
    scale = lax.rsqrt(jnp.mean(floats * floats, axis=1, keepdims=True) + EPSILON)
    slot = lax.broadcasted_iota(jnp.int32, (slots, rows), 0)
    expert = sum((slot >= CAP * e).astype(jnp.int32) for e in range(1, EXPERTS))
    wanted = (slot - expert * CAP).astype(f32)
    first = ids[0:1, :] == expert
    second = ids[1:2, :] == expert
    named = jnp.where(jnp.logical_or(first, second), 1.0, 0.0)
    before = jnp.where(
        lax.broadcasted_iota(jnp.int32, (rows, rows), 0)
        < lax.broadcasted_iota(jnp.int32, (rows, rows), 1),
        1.0,
        0.0,
    ).astype(bf16)
    position = jnp.dot(named.astype(bf16), before, preferred_element_type=f32)
    picker = jnp.where(position == wanted, named, 0.0)
    gate = jnp.where(first, gates[0:1, :], jnp.where(second, gates[1:2, :], 0.0))
    combine[...] = picker * gate
    start = pl.multiple_of((lax.axis_index("x") * CORES + lax.axis_index("core")) * width, width)
    mine = tokens[:, pl.ds(start, width)]
    residual[...] = mine
    normed = (mine.astype(f32) * scale).astype(bf16)
    total = jnp.dot(picker.astype(bf16), normed, preferred_element_type=f32).astype(bf16)
    copies = packed.shape[0] // EXPERTS
    for e in range(EXPERTS):
        for copy in range(copies):
            packed[e * copies + copy] = total[e * CAP : (e + 1) * CAP]


def pack(tokens, ids, gates, far, width):
    rows = tokens.shape[0]
    arrays = (tokens, ids.T, gates.T)
    return pl.pallas_call(
        pack_kernel,
        compiler_params=PARAMS,
        in_specs=[whole(pltpu.HBM)] * 3,
        out_specs=[whole()] * 3,
        out_shape=[
            pltpu.VMEM((far, CAP, width), jnp.bfloat16),
            pltpu.VMEM((EXPERTS * CAP, rows), jnp.float32),
            pltpu.VMEM((rows, width), jnp.bfloat16),
        ],
        scratch_shapes=[pltpu.VMEM(array.shape, array.dtype) for array in arrays]
        + [pltpu.SemaphoreType.DMA((3,))],
    )(*[pltpu.with_memory_space_constraint(array, pltpu.HBM) for array in arrays])


def product_kernel(own, other, *refs):
    count = (len(refs) - 2) // 2
    sources, out, held, sems = refs[:count], refs[count], refs[count + 1 : -1], refs[-1]
    moves = [
        pltpu.make_async_copy(source, place, sems.at[shift])
        for shift, (source, place) in enumerate(zip(sources, held))
    ]
    for move in moves:
        move.start()
    x, core = lax.axis_index("x"), lax.axis_index("core")
    width, depth = out.shape[-1], own.shape[1]
    for shift in range(count):
        moves[shift].wait()
        to = lax.rem(x + (count - shift), count)
        product = 0.0
        for left, side in ((own, core), (other, 1 - core)):
            at = pl.multiple_of(side * depth, depth)
            both = jnp.concatenate(
                [held[shift][kind, pl.ds(at, depth), :] for kind in range(2)], axis=1
            )
            product = product + jnp.dot(left[...], both, preferred_element_type=jnp.float32)
        product = product.astype(out.dtype)
        for kind in range(2):
            out[to, kind] = product[:, kind * width : (kind + 1) * width]


def products(own, other, chunks):
    xs, n_rows, width = len(chunks), own.shape[0], chunks[0].shape[2]
    chunks = [pltpu.with_memory_space_constraint(chunk, pltpu.HBM) for chunk in chunks]
    return pl.pallas_call(
        product_kernel,
        compiler_params=PARAMS,
        in_specs=[whole()] * 2 + [whole(pltpu.HBM)] * xs,
        out_specs=whole(),
        out_shape=pltpu.VMEM((xs, 2, n_rows, width), jnp.bfloat16),
        scratch_shapes=[pltpu.VMEM(chunk.shape, chunk.dtype) for chunk in chunks]
        + [pltpu.SemaphoreType.DMA((xs,))],
    )(*near_memory(own, other), *chunks)


def hidden_kernel(sums, out):
    f32 = jnp.float32
    block = sums.shape[2] // (NEAR * CORES)
    for line in range(NEAR):
        for side in range(CORES):
            at = (line * CORES + side) * block
            total = sums[0, :, at : at + block, :].astype(f32)
            for source in range(1, sums.shape[0]):
                total = total + sums[source, :, at : at + block, :].astype(f32)
            gate, up = total[0], total[1]
            hidden = (gate / (1.0 + jnp.exp(-gate)) * up).astype(out.dtype)
            for copy in range(out.shape[0] // CORES):
                out[copy * CORES + side, line * block : (line + 1) * block, :] = hidden


def hidden_units(sums):
    xs, _, n_rows, width = sums.shape
    return pl.pallas_call(
        hidden_kernel,
        compiler_params=PARAMS,
        in_specs=[whole()],
        out_specs=whole(),
        out_shape=pltpu.VMEM((xs * CORES, n_rows // CORES, width), jnp.bfloat16),
    )(*near_memory(sums))


def down_kernel(units, own, other, out):
    near, _, block, _ = out.shape
    core = lax.axis_index("core")
    left = jnp.concatenate([units[source] for source in range(units.shape[0])], axis=1)
    for side, weight in ((core, own), (1 - core, other)):
        product = jnp.dot(left, weight[...], preferred_element_type=jnp.float32).astype(out.dtype)
        for line in range(near):
            out[line, side] = product[line * block : (line + 1) * block]


def down(units, own, other, near):
    n_rows = units.shape[1]
    return pl.pallas_call(
        down_kernel,
        compiler_params=PARAMS,
        in_specs=[whole()] * 3,
        out_specs=whole(),
        out_shape=pltpu.VMEM((near, CORES, n_rows // near, own.shape[1]), jnp.bfloat16),
    )(*near_memory(units, own, other))


def layer(tokens, route_ids, route_gates, gate_weight, up_weight, down_weight):
    f32, bf16 = jnp.float32, jnp.bfloat16
    model_width = tokens.shape[1]
    far, near, xs = lax.axis_size("far"), lax.axis_size("near"), lax.axis_size("x")
    x = lax.axis_index("x")
    chip_width = model_width // xs
    out_width = down_weight.shape[1]
    copies = far // EXPERTS
    swap = [(i, (i + 1) % CORES) for i in range(CORES)]
    sent, combine, residual = pack(tokens, route_ids, route_gates, far, out_width)
    arrived = lax.all_to_all(sent, "far", 0, 0, tiled=True)

    def chunk(shift):
        start = (x + shift) % xs * chip_width
        return jnp.stack(
            [
                lax.dynamic_slice_in_dim(weight, start, chip_width, 0)
                for weight in (gate_weight, up_weight)
            ]
        )

    chunks = [chunk(0)]
    for shift in range(1, xs):
        chunks.append(lax.ppermute(chunk(shift), "x", [(i, (i + shift) % xs) for i in range(xs)]))
    down_other = lax.ppermute(down_weight, "core", swap)

    arrived = arrived.reshape(far, CORES, PART, out_width)
    arrived = jnp.swapaxes(arrived, 0, 1).reshape(far * CAP, out_width)
    rows = lax.all_gather(arrived, "near", axis=0, tiled=True)
    rows_other = lax.ppermute(rows, "core", swap)
    sums = lax.all_to_all(products(rows, rows_other, chunks), "x", 0, 0, tiled=True)
    units = lax.all_to_all(hidden_units(sums), ("x", "core"), 0, 0, tiled=True)
    produced = down(units, down_weight, down_other, near)
    parts = lax.all_to_all(
        produced.reshape(near * CORES, far * PART, out_width), ("near", "core"), 0, 0, tiled=True
    )
    summed = jnp.sum(
        parts.reshape(near, CORES, far, PART, out_width).astype(f32), axis=0
    ).astype(bf16)
    summed = jnp.swapaxes(summed, 0, 1).reshape(far, CAP, out_width)
    returned = lax.all_to_all(summed, "far", 0, 0, tiled=True)
    returned = jnp.sum(
        returned.reshape(EXPERTS, copies, CAP, out_width).astype(f32), axis=1
    ).reshape(EXPERTS * CAP, out_width)
    mixture = jnp.einsum(
        "st,sd->td",
        combine,
        returned,
        precision=lax.Precision.HIGHEST,
        preferred_element_type=f32,
    )
    return (residual.astype(f32) + mixture).astype(bf16)


def solution(mesh):
    groups, experts, tensor = (mesh.shape[n] for n in ("groups", "expert", "tensor"))
    fine = Mesh(
        mesh.devices.reshape(groups, experts // NEAR, NEAR, tensor // CORES, CORES),
        ("groups", "far", "near", "x", "core"),
    )
    tok = ("groups", "far", "near")
    in_specs = (
        P(tok, None),
        P(tok, None),
        P(tok, None),
        P(None, ("far", "near", "x", "core")),
        P(None, ("far", "near", "x", "core")),
        P(("far", "near"), ("x", "core")),
    )
    out_specs = P(tok, ("x", "core"))
    return jax.shard_map(layer, mesh=fine, in_specs=in_specs, out_specs=out_specs, check_vma=False)
```

```python
import jax
import jax.numpy as jnp
from jax import lax
from jax.experimental import pallas as pl
from jax.experimental.pallas import tpu as pltpu
from jax.sharding import Mesh, PartitionSpec as P


EXPERTS = 4
CAP = 24
NEAR = 4
CORES = 2
PART = CAP // CORES

EPSILON = 1e-05


def whole(space=None):
    return pl.BlockSpec(memory_space=space or pltpu.VMEM)


PARAMS = pltpu.CompilerParams(vmem_limit_bytes=16 << 20)


def near_memory(*arrays):
    return [pltpu.with_memory_space_constraint(array, pltpu.VMEM) for array in arrays]


def pack_kernel(*refs):
    sources, (packed, combine, residual), held, sems = refs[:3], refs[3:6], refs[6:9], refs[9]
    moves = [
        pltpu.make_async_copy(source, place, sems.at[number])
        for number, (source, place) in enumerate(zip(sources, held))
    ]
    for move in moves:
        move.start()
    for move in moves:
        move.wait()
    tokens, ids, gates = held
    f32, bf16 = jnp.float32, jnp.bfloat16
    half = packed.shape[2]
    rows = tokens.shape[0]
    x, core = lax.axis_index("x"), lax.axis_index("core")
    out_width = residual.shape[1]
    floats = tokens[...].astype(f32)
    scale = lax.rsqrt(jnp.mean(floats * floats, axis=1, keepdims=True) + EPSILON)
    before = jnp.where(
        lax.broadcasted_iota(jnp.int32, (rows, rows), 0)
        < lax.broadcasted_iota(jnp.int32, (rows, rows), 1),
        1.0,
        0.0,
    ).astype(bf16)
    lines = EXPERTS * CAP
    line = lax.broadcasted_iota(jnp.int32, (lines, rows), 0)
    expert = sum((line >= CAP * e).astype(jnp.int32) for e in range(1, EXPERTS))
    at = line - expert * CAP
    first = ids[0:1, :] == expert
    second = ids[1:2, :] == expert
    named = jnp.where(jnp.logical_or(first, second), 1.0, 0.0)
    position = jnp.dot(named.astype(bf16), before, preferred_element_type=f32)
    gate = jnp.where(first, gates[0:1, :], jnp.where(second, gates[1:2, :], 0.0))
    combine[...] = jnp.where(position == at.astype(f32), gate, 0.0)
    upper = (at >= PART).astype(jnp.int32)
    wanted = (at - upper * PART + core * PART).astype(f32)
    picker = jnp.where(position == wanted, named, 0.0)
    total = jnp.zeros((lines, half), f32)
    for part in range(2):
        start = pl.multiple_of((x * 2 + part) * half, half)
        normed = (tokens[:, pl.ds(start, half)].astype(f32) * scale).astype(bf16)
        mine = jnp.where(upper == part, picker, 0.0).astype(bf16)
        total = total + jnp.dot(mine, normed, preferred_element_type=f32)
    total = total.astype(bf16)
    copies = packed.shape[0] // EXPERTS
    for e in range(EXPERTS):
        for copy in range(copies):
            packed[e * copies + copy] = total[e * CAP : (e + 1) * CAP]
    start = pl.multiple_of((x * CORES + core) * out_width, out_width)
    residual[...] = tokens[:, pl.ds(start, out_width)]


def pack(tokens, ids, gates, far, chip_width, out_width):
    rows = tokens.shape[0]
    arrays = (tokens, ids.T, gates.T)
    return pl.pallas_call(
        pack_kernel,
        compiler_params=PARAMS,
        in_specs=[whole(pltpu.HBM)] * 3,
        out_specs=[whole()] * 3,
        out_shape=[
            pltpu.VMEM((far, CAP, chip_width // 2), jnp.bfloat16),
            pltpu.VMEM((EXPERTS * CAP, rows), jnp.float32),
            pltpu.VMEM((rows, out_width), jnp.bfloat16),
        ],
        scratch_shapes=[pltpu.VMEM(array.shape, array.dtype) for array in arrays]
        + [pltpu.SemaphoreType.DMA((3,))],
    )(*[pltpu.with_memory_space_constraint(array, pltpu.HBM) for array in arrays])


def product_kernel(rows, own, other, out, held, sem):
    xs, kinds, _, width = own.shape
    move = pltpu.make_async_copy(other, held, sem)
    move.start()
    x = lax.axis_index("x")
    left = rows[...]
    for core, weights in enumerate((own, held)):
        if core:
            move.wait()
        for shift in range(xs):
            to = lax.rem(x + (xs - shift), xs)
            both = jnp.concatenate([weights[shift, kind] for kind in range(kinds)], axis=1)
            product = jnp.dot(left, both, preferred_element_type=jnp.float32).astype(out.dtype)
            for kind in range(kinds):
                out[to, core, kind] = product[:, kind * width : (kind + 1) * width]


def products(rows, own, other):
    n_rows = rows.shape[0]
    xs, kinds, _, width = own.shape
    return pl.pallas_call(
        product_kernel,
        compiler_params=PARAMS,
        in_specs=[whole(), whole(), whole(pltpu.HBM)],
        out_specs=whole(),
        out_shape=pltpu.VMEM((xs, CORES, kinds, n_rows, width), jnp.bfloat16),
        scratch_shapes=[pltpu.VMEM(other.shape, other.dtype), pltpu.SemaphoreType.DMA],
    )(*near_memory(rows, own), pltpu.with_memory_space_constraint(other, pltpu.HBM))


def hidden_kernel(sums, out):
    f32 = jnp.float32
    xs, _, _, n_rows, width = sums.shape
    straight = lax.axis_index("core") == 0
    block = 32
    for at in range(0, n_rows, block):
        total = sums[0, :, :, at : at + block, :].astype(f32)
        for source in range(1, xs):
            total = total + sums[source, :, :, at : at + block, :].astype(f32)
        gate, up = total[:, 0], total[:, 1]
        hidden = (gate / (1.0 + jnp.exp(-gate)) * up).astype(out.dtype)
        low = jnp.where(straight, hidden[0], hidden[1])
        high = jnp.where(straight, hidden[1], hidden[0])
        for copy in range(out.shape[0]):
            out[copy, at : at + block, 0:width] = low
            out[copy, at : at + block, width : 2 * width] = high


def hidden_units(sums):
    xs, cores, _, n_rows, width = sums.shape
    return pl.pallas_call(
        hidden_kernel,
        compiler_params=PARAMS,
        in_specs=[whole()],
        out_specs=whole(),
        out_shape=pltpu.VMEM((xs, n_rows, cores * width), jnp.bfloat16),
    )(*near_memory(sums))


def down_kernel(units, own, other, out):
    near, _, block, _ = out.shape
    core = lax.axis_index("core")
    left = jnp.concatenate([units[source] for source in range(units.shape[0])], axis=1)
    for side, weight in ((core, own), (1 - core, other)):
        product = jnp.dot(left, weight[...], preferred_element_type=jnp.float32).astype(out.dtype)
        for line in range(near):
            out[line, side] = product[line * block : (line + 1) * block]


def down(units, own, other, near):
    n_rows = units.shape[1]
    return pl.pallas_call(
        down_kernel,
        compiler_params=PARAMS,
        in_specs=[whole()] * 3,
        out_specs=whole(),
        out_shape=pltpu.VMEM((near, CORES, n_rows // near, own.shape[1]), jnp.bfloat16),
    )(*near_memory(units, own, other))


def layer(tokens, route_ids, route_gates, gate_weight, up_weight, down_weight):
    f32, bf16 = jnp.float32, jnp.bfloat16
    model_width = tokens.shape[1]
    far, near, xs = lax.axis_size("far"), lax.axis_size("near"), lax.axis_size("x")
    x = lax.axis_index("x")
    chip_width = model_width // xs
    out_width = down_weight.shape[1]
    copies = far // EXPERTS
    swap = [(i, (i + 1) % CORES) for i in range(CORES)]
    sent, combine, residual = pack(tokens, route_ids, route_gates, far, chip_width, out_width)
    arrived = lax.all_to_all(sent, "far", 0, 0, tiled=True)

    def chunk(shift):
        start = (x + shift) % xs * chip_width
        return jnp.stack(
            [
                lax.dynamic_slice_in_dim(weight, start, chip_width, 0)
                for weight in (gate_weight, up_weight)
            ]
        )

    chunks = [chunk(0)]
    for shift in range(1, xs):
        chunks.append(lax.ppermute(chunk(shift), "x", [(i, (i + shift) % xs) for i in range(xs)]))
    own = jnp.stack(chunks)
    other = lax.ppermute(own, "core", swap)
    down_other = lax.ppermute(down_weight, "core", swap)

    arrived = arrived.reshape(far, 2, PART, chip_width // 2)
    arrived = jnp.swapaxes(arrived, 1, 2).reshape(1, far * PART, chip_width)
    rows = lax.all_to_all(
        jnp.broadcast_to(arrived, (near, far * PART, chip_width)), "near", 0, 0, tiled=True
    )
    n_rows = near * far * PART
    partial = products(rows.reshape(n_rows, chip_width), own, other)
    sums = lax.all_to_all(partial, "x", 0, 0, tiled=True)
    units = lax.all_to_all(hidden_units(sums), "x", 0, 0, tiled=True)
    produced = down(units, down_weight, down_other, near)
    parts = lax.all_to_all(
        produced.reshape(near * CORES, far * PART, out_width), ("near", "core"), 0, 0, tiled=True
    )
    summed = jnp.sum(
        parts.reshape(near, CORES, far, PART, out_width).astype(f32), axis=0
    ).astype(bf16)
    summed = jnp.swapaxes(summed, 0, 1).reshape(far, CAP, out_width)
    returned = lax.all_to_all(summed, "far", 0, 0, tiled=True)
    returned = jnp.sum(
        returned.reshape(EXPERTS, copies, CAP, out_width).astype(f32), axis=1
    ).reshape(EXPERTS * CAP, out_width)
    mixture = jnp.einsum(
        "st,sd->td",
        combine,
        returned,
        precision=lax.Precision.HIGHEST,
        preferred_element_type=f32,
    )
    return (residual.astype(f32) + mixture).astype(bf16)


def solution(mesh):
    groups, experts, tensor = (mesh.shape[n] for n in ("groups", "expert", "tensor"))
    fine = Mesh(
        mesh.devices.reshape(groups, experts // NEAR, NEAR, tensor // CORES, CORES),
        ("groups", "far", "near", "x", "core"),
    )
    tok = ("groups", "far", "near")
    in_specs = (
        P(tok, None),
        P(tok, None),
        P(tok, None),
        P(None, ("far", "near", "x", "core")),
        P(None, ("far", "near", "x", "core")),
        P(("far", "near"), ("x", "core")),
    )
    out_specs = P(tok, ("x", "core"))
    return jax.shard_map(layer, mesh=fine, in_specs=in_specs, out_specs=out_specs, check_vma=False)
```

```python
import jax
import jax.numpy as jnp
from jax import lax
from jax.experimental import pallas as pl
from jax.experimental.pallas import tpu as pltpu
from jax.sharding import Mesh, PartitionSpec as P


EXPERTS = 4
CAP = 24
NEAR = 8
CORES = 2
PART = CAP // CORES

EPSILON = 1e-05


def whole(space=None):
    return pl.BlockSpec(memory_space=space or pltpu.VMEM)


PARAMS = pltpu.CompilerParams(vmem_limit_bytes=16 << 20)


def near_memory(*arrays):
    return [pltpu.with_memory_space_constraint(array, pltpu.VMEM) for array in arrays]


def pack_kernel(*refs):
    sources, (packed, combine, residual), held, sems = refs[:3], refs[3:6], refs[6:9], refs[9]
    moves = [
        pltpu.make_async_copy(source, place, sems.at[number])
        for number, (source, place) in enumerate(zip(sources, held))
    ]
    for move in moves:
        move.start()
    for move in moves:
        move.wait()
    tokens, ids, gates = held
    f32, bf16 = jnp.float32, jnp.bfloat16
    half = packed.shape[2]
    rows = tokens.shape[0]
    x, core = lax.axis_index("x"), lax.axis_index("core")
    out_width = residual.shape[1]
    floats = tokens[...].astype(f32)
    scale = lax.rsqrt(jnp.mean(floats * floats, axis=1, keepdims=True) + EPSILON)
    before = jnp.where(
        lax.broadcasted_iota(jnp.int32, (rows, rows), 0)
        < lax.broadcasted_iota(jnp.int32, (rows, rows), 1),
        1.0,
        0.0,
    ).astype(bf16)
    lines = EXPERTS * CAP
    line = lax.broadcasted_iota(jnp.int32, (lines, rows), 0)
    expert = sum((line >= CAP * e).astype(jnp.int32) for e in range(1, EXPERTS))
    at = line - expert * CAP
    first = ids[0:1, :] == expert
    second = ids[1:2, :] == expert
    named = jnp.where(jnp.logical_or(first, second), 1.0, 0.0)
    position = jnp.dot(named.astype(bf16), before, preferred_element_type=f32)
    gate = jnp.where(first, gates[0:1, :], jnp.where(second, gates[1:2, :], 0.0))
    combine[...] = jnp.where(position == at.astype(f32), gate, 0.0)
    upper = (at >= PART).astype(jnp.int32)
    wanted = (at - upper * PART + core * PART).astype(f32)
    picker = jnp.where(position == wanted, named, 0.0)
    total = jnp.zeros((lines, half), f32)
    for part in range(2):
        start = pl.multiple_of((x * 2 + part) * half, half)
        normed = (tokens[:, pl.ds(start, half)].astype(f32) * scale).astype(bf16)
        mine = jnp.where(upper == part, picker, 0.0).astype(bf16)
        total = total + jnp.dot(mine, normed, preferred_element_type=f32)
    total = total.astype(bf16)
    copies = packed.shape[0] // EXPERTS
    for e in range(EXPERTS):
        for copy in range(copies):
            packed[e * copies + copy] = total[e * CAP : (e + 1) * CAP]
    start = pl.multiple_of((x * CORES + core) * out_width, out_width)
    residual[...] = tokens[:, pl.ds(start, out_width)]


def pack(tokens, ids, gates, far, chip_width, out_width):
    rows = tokens.shape[0]
    arrays = (tokens, ids.T, gates.T)
    return pl.pallas_call(
        pack_kernel,
        compiler_params=PARAMS,
        in_specs=[whole(pltpu.HBM)] * 3,
        out_specs=[whole()] * 3,
        out_shape=[
            pltpu.VMEM((far, CAP, chip_width // 2), jnp.bfloat16),
            pltpu.VMEM((EXPERTS * CAP, rows), jnp.float32),
            pltpu.VMEM((rows, out_width), jnp.bfloat16),
        ],
        scratch_shapes=[pltpu.VMEM(array.shape, array.dtype) for array in arrays]
        + [pltpu.SemaphoreType.DMA((3,))],
    )(*[pltpu.with_memory_space_constraint(array, pltpu.HBM) for array in arrays])


def product_kernel(rows, own, other, out, held, sem):
    xs, kinds, _, width = own.shape
    moves = [
        pltpu.make_async_copy(other.at[shift], held.at[shift], sem.at[shift])
        for shift in range(xs)
    ]
    for move in moves:
        move.start()
    x = lax.axis_index("x")
    left = rows[...]
    for core, weights in enumerate((own, held)):
        for shift in range(xs):
            if core:
                moves[shift].wait()
            to = lax.rem(x + (xs - shift), xs)
            both = jnp.concatenate([weights[shift, kind] for kind in range(kinds)], axis=1)
            product = jnp.dot(left, both, preferred_element_type=jnp.float32).astype(out.dtype)
            for kind in range(kinds):
                out[to, core, kind] = product[:, kind * width : (kind + 1) * width]


def products(rows, own, other):
    n_rows = rows.shape[0]
    xs, kinds, _, width = own.shape
    return pl.pallas_call(
        product_kernel,
        compiler_params=PARAMS,
        in_specs=[whole(), whole(), whole(pltpu.HBM)],
        out_specs=whole(),
        out_shape=pltpu.VMEM((xs, CORES, kinds, n_rows, width), jnp.bfloat16),
        scratch_shapes=[pltpu.VMEM(other.shape, other.dtype), pltpu.SemaphoreType.DMA((xs,))],
    )(*near_memory(rows, own), pltpu.with_memory_space_constraint(other, pltpu.HBM))


def hidden_kernel(sums, *refs):
    sources, out, places, sems = refs[:CORES], refs[CORES], refs[CORES + 1 : -1], refs[-1]
    moves = [
        pltpu.make_async_copy(source, place, sems.at[number])
        for number, (source, place) in enumerate(zip(sources, places))
    ]
    for move in moves:
        move.start()
    f32 = jnp.float32
    xs, _, _, n_rows, width = sums.shape
    straight = lax.axis_index("core") == 0
    block = 32
    for at in range(0, n_rows, block):
        total = sums[0, :, :, at : at + block, :].astype(f32)
        for source in range(1, xs):
            total = total + sums[source, :, :, at : at + block, :].astype(f32)
        gate, up = total[:, 0], total[:, 1]
        hidden = (gate / (1.0 + jnp.exp(-gate)) * up).astype(out.dtype)
        low = jnp.where(straight, hidden[0], hidden[1])
        high = jnp.where(straight, hidden[1], hidden[0])
        for copy in range(out.shape[0]):
            out[copy, at : at + block, 0:width] = low
            out[copy, at : at + block, width : 2 * width] = high
    for move in moves:
        move.wait()


def hidden_units(sums, *weights):
    xs, cores, _, n_rows, width = sums.shape
    far_weights = [pltpu.with_memory_space_constraint(weight, pltpu.HBM) for weight in weights]
    return pl.pallas_call(
        hidden_kernel,
        compiler_params=PARAMS,
        in_specs=[whole()] + [whole(pltpu.HBM)] * CORES,
        out_specs=[whole()] * (1 + CORES),
        out_shape=[pltpu.VMEM((xs, n_rows, cores * width), jnp.bfloat16)]
        + [pltpu.VMEM(weight.shape, weight.dtype) for weight in weights],
        scratch_shapes=[pltpu.SemaphoreType.DMA((CORES,))],
    )(*near_memory(sums), *far_weights)


def down_kernel(units, own, other, out):
    near, _, block, _ = out.shape
    core = lax.axis_index("core")
    left = jnp.concatenate([units[source] for source in range(units.shape[0])], axis=1)
    for side, weight in ((core, own), (1 - core, other)):
        product = jnp.dot(left, weight[...], preferred_element_type=jnp.float32).astype(out.dtype)
        for line in range(near):
            out[line, side] = product[line * block : (line + 1) * block]


def down(units, own, other, near):
    n_rows = units.shape[1]
    return pl.pallas_call(
        down_kernel,
        compiler_params=PARAMS,
        in_specs=[whole()] * 3,
        out_specs=whole(),
        out_shape=pltpu.VMEM((near, CORES, n_rows // near, own.shape[1]), jnp.bfloat16),
    )(*near_memory(units, own, other))


def layer(tokens, route_ids, route_gates, gate_weight, up_weight, down_weight):
    f32, bf16 = jnp.float32, jnp.bfloat16
    model_width = tokens.shape[1]
    far, near, xs = lax.axis_size("far"), lax.axis_size("near"), lax.axis_size("x")
    x = lax.axis_index("x")
    chip_width = model_width // xs
    out_width = down_weight.shape[1]
    copies = far // EXPERTS
    swap = [(i, (i + 1) % CORES) for i in range(CORES)]
    sent, combine, residual = pack(tokens, route_ids, route_gates, far, chip_width, out_width)
    arrived = lax.all_to_all(sent, "far", 0, 0, tiled=True)

    def chunk(shift):
        start = (x + shift) % xs * chip_width
        return jnp.stack(
            [
                lax.dynamic_slice_in_dim(weight, start, chip_width, 0)
                for weight in (gate_weight, up_weight)
            ]
        )

    chunks = [chunk(0)]
    for shift in range(1, xs):
        chunks.append(lax.ppermute(chunk(shift), "x", [(i, (i + shift) % xs) for i in range(xs)]))
    own = jnp.stack(chunks)
    other = lax.ppermute(own, "core", swap)
    down_other = lax.ppermute(down_weight, "core", swap)

    arrived = arrived.reshape(far, 2, PART, chip_width // 2)
    arrived = jnp.swapaxes(arrived, 1, 2).reshape(1, far * PART, chip_width)
    rows = lax.all_to_all(
        jnp.broadcast_to(arrived, (near, far * PART, chip_width)), "near", 0, 0, tiled=True
    )
    n_rows = near * far * PART
    rows, down_other = lax.optimization_barrier((rows, down_other))
    partial = products(rows.reshape(n_rows, chip_width), own, other)
    sums = lax.all_to_all(partial, "x", 0, 0, tiled=True)
    hidden, down_weight, down_other = hidden_units(sums, down_weight, down_other)
    units = lax.all_to_all(hidden, "x", 0, 0, tiled=True)
    produced = down(units, down_weight, down_other, near)
    parts = lax.all_to_all(
        produced.reshape(near * CORES, far * PART, out_width), ("near", "core"), 0, 0, tiled=True
    )
    summed = jnp.sum(
        parts.reshape(near, CORES, far, PART, out_width).astype(f32), axis=0
    ).astype(bf16)
    summed = jnp.swapaxes(summed, 0, 1).reshape(far, CAP, out_width)
    returned = lax.all_to_all(summed, "far", 0, 0, tiled=True)
    returned = jnp.sum(
        returned.reshape(EXPERTS, copies, CAP, out_width).astype(f32), axis=1
    ).reshape(EXPERTS * CAP, out_width)
    mixture = jnp.einsum(
        "st,sd->td",
        combine,
        returned,
        precision=lax.Precision.HIGHEST,
        preferred_element_type=f32,
    )
    return (residual.astype(f32) + mixture).astype(bf16)


def solution(mesh):
    groups, experts, tensor = (mesh.shape[n] for n in ("groups", "expert", "tensor"))
    fine = Mesh(
        mesh.devices.reshape(groups, experts // NEAR, NEAR, tensor // CORES, CORES),
        ("groups", "far", "near", "x", "core"),
    )
    tok = ("groups", "far", "near")
    in_specs = (
        P(tok, None),
        P(tok, None),
        P(tok, None),
        P(None, ("far", "near", "x", "core")),
        P(None, ("far", "near", "x", "core")),
        P(("far", "near"), ("x", "core")),
    )
    out_specs = P(tok, ("x", "core"))
    return jax.shard_map(layer, mesh=fine, in_specs=in_specs, out_specs=out_specs, check_vma=False)
```

```python
import jax
import jax.numpy as jnp
from jax import lax
from jax.experimental import pallas as pl
from jax.experimental.pallas import tpu as pltpu
from jax.sharding import Mesh, PartitionSpec as P


EXPERTS = 4
CAP = 24
NEAR = 4
CORES = 2
PART = CAP // CORES

EPSILON = 1e-05


def whole(space=None):
    return pl.BlockSpec(memory_space=space or pltpu.VMEM)


PARAMS = pltpu.CompilerParams(vmem_limit_bytes=16 << 20)


def near_memory(*arrays):
    return [pltpu.with_memory_space_constraint(array, pltpu.VMEM) for array in arrays]


def pack_kernel(*refs):
    sources, (packed, combine, residual), held, sems = refs[:3], refs[3:6], refs[6:9], refs[9]
    moves = [
        pltpu.make_async_copy(source, place, sems.at[number])
        for number, (source, place) in enumerate(zip(sources, held))
    ]
    for move in moves:
        move.start()
    for move in moves:
        move.wait()
    tokens, ids, gates = held
    f32, bf16 = jnp.float32, jnp.bfloat16
    half = packed.shape[2]
    rows = tokens.shape[0]
    x, core = lax.axis_index("x"), lax.axis_index("core")
    out_width = residual.shape[1]
    floats = tokens[...].astype(f32)
    scale = lax.rsqrt(jnp.mean(floats * floats, axis=1, keepdims=True) + EPSILON)
    before = jnp.where(
        lax.broadcasted_iota(jnp.int32, (rows, rows), 0)
        < lax.broadcasted_iota(jnp.int32, (rows, rows), 1),
        1.0,
        0.0,
    ).astype(bf16)
    lines = EXPERTS * CAP
    line = lax.broadcasted_iota(jnp.int32, (lines, rows), 0)
    expert = sum((line >= CAP * e).astype(jnp.int32) for e in range(1, EXPERTS))
    at = line - expert * CAP
    first = ids[0:1, :] == expert
    second = ids[1:2, :] == expert
    named = jnp.where(jnp.logical_or(first, second), 1.0, 0.0)
    position = jnp.dot(named.astype(bf16), before, preferred_element_type=f32)
    gate = jnp.where(first, gates[0:1, :], jnp.where(second, gates[1:2, :], 0.0))
    combine[...] = jnp.where(position == at.astype(f32), gate, 0.0)
    upper = (at >= PART).astype(jnp.int32)
    wanted = (at - upper * PART + core * PART).astype(f32)
    picker = jnp.where(position == wanted, named, 0.0)
    total = jnp.zeros((lines, half), f32)
    for part in range(2):
        start = pl.multiple_of((x * 2 + part) * half, half)
        normed = (tokens[:, pl.ds(start, half)].astype(f32) * scale).astype(bf16)
        mine = jnp.where(upper == part, picker, 0.0).astype(bf16)
        total = total + jnp.dot(mine, normed, preferred_element_type=f32)
    total = total.astype(bf16)
    copies = packed.shape[0] // EXPERTS
    for e in range(EXPERTS):
        for copy in range(copies):
            packed[e * copies + copy] = total[e * CAP : (e + 1) * CAP]
    start = pl.multiple_of((x * CORES + core) * out_width, out_width)
    residual[...] = tokens[:, pl.ds(start, out_width)]


def pack(tokens, ids, gates, far, chip_width, out_width):
    rows = tokens.shape[0]
    arrays = (tokens, ids.T, gates.T)
    return pl.pallas_call(
        pack_kernel,
        compiler_params=PARAMS,
        in_specs=[whole(pltpu.HBM)] * 3,
        out_specs=[whole()] * 3,
        out_shape=[
            pltpu.VMEM((far, CAP, chip_width // 2), jnp.bfloat16),
            pltpu.VMEM((EXPERTS * CAP, rows), jnp.float32),
            pltpu.VMEM((rows, out_width), jnp.bfloat16),
        ],
        scratch_shapes=[pltpu.VMEM(array.shape, array.dtype) for array in arrays]
        + [pltpu.SemaphoreType.DMA((3,))],
    )(*[pltpu.with_memory_space_constraint(array, pltpu.HBM) for array in arrays])


def own_kernel(rows, *refs):
    chunks, out, stacked, sems = refs[:-3], refs[-3], refs[-2], refs[-1]
    xs, width = len(chunks), out.shape[-1]
    moves = [
        pltpu.make_async_copy(weights, stacked.at[shift], sems.at[shift])
        for shift, weights in enumerate(chunks)
    ]
    for move in moves:
        move.start()
    x = lax.axis_index("x")
    left = rows[...]
    for shift, weights in enumerate(chunks):
        to = lax.rem(x + (xs - shift), xs)
        gate, up = weights[0], weights[1]
        product = jnp.dot(
            left, jnp.concatenate([gate, up], axis=1), preferred_element_type=jnp.float32
        ).astype(out.dtype)
        out[to, 0] = product[:, :width]
        out[to, 1] = product[:, width:]
    for move in moves:
        move.wait()


def own_products(rows, chunks):
    xs, n_rows = len(chunks), rows.shape[0]
    return pl.pallas_call(
        own_kernel,
        compiler_params=PARAMS,
        in_specs=[whole()] * (1 + xs),
        out_specs=[whole(), whole(pltpu.HBM)],
        out_shape=[
            pltpu.VMEM((xs, 2, n_rows, chunks[0].shape[2]), jnp.bfloat16),
            pltpu.HBM((xs, *chunks[0].shape), jnp.bfloat16),
        ],
        scratch_shapes=[pltpu.SemaphoreType.DMA((xs,))],
    )(rows, *chunks)


def other_kernel(rows, stacked, out):
    xs, _, _, width = stacked.shape
    x = lax.axis_index("x")
    left = rows[...]
    for shift in range(xs):
        to = lax.rem(x + (xs - shift), xs)
        both = jnp.concatenate([stacked[shift, 0], stacked[shift, 1]], axis=1)
        product = jnp.dot(left, both, preferred_element_type=jnp.float32).astype(out.dtype)
        out[to, 0] = product[:, :width]
        out[to, 1] = product[:, width:]


def other_products(rows, stacked):
    xs, _, _, width = stacked.shape
    return pl.pallas_call(
        other_kernel,
        compiler_params=PARAMS,
        in_specs=[whole()] * 2,
        out_specs=whole(),
        out_shape=pltpu.VMEM((xs, 2, rows.shape[0], width), jnp.bfloat16),
    )(rows, stacked)


def hidden_of(sums, at, block, dtype):
    f32 = jnp.float32
    total = sums[0, :, at : at + block, :].astype(f32)
    for source in range(1, sums.shape[0]):
        total = total + sums[source, :, at : at + block, :].astype(f32)
    gate, up = total[0], total[1]
    return (gate / (1.0 + jnp.exp(-gate)) * up).astype(dtype)


def first_kernel(sums, out):
    block = 64
    for at in range(0, out.shape[0], block):
        out[at : at + block, :] = hidden_of(sums, at, block, out.dtype)


def first_units(sums):
    return pl.pallas_call(
        first_kernel,
        compiler_params=PARAMS,
        in_specs=[whole()],
        out_specs=whole(),
        out_shape=pltpu.VMEM(sums.shape[2:], jnp.bfloat16),
    )(*near_memory(sums))


def hidden_kernel(sums, *refs):
    sources, out, places, sems = refs[:CORES], refs[CORES], refs[CORES + 1 : -1], refs[-1]
    moves = [
        pltpu.make_async_copy(source, place, sems.at[number])
        for number, (source, place) in enumerate(zip(sources, places))
    ]
    for move in moves:
        move.start()
    block = 64
    for at in range(0, out.shape[1], block):
        hidden = hidden_of(sums, at, block, out.dtype)
        for copy in range(out.shape[0]):
            out[copy, at : at + block, :] = hidden
    for move in moves:
        move.wait()


def hidden_units(sums, *weights):
    xs, _, n_rows, width = sums.shape
    far_weights = [pltpu.with_memory_space_constraint(weight, pltpu.HBM) for weight in weights]
    return pl.pallas_call(
        hidden_kernel,
        compiler_params=PARAMS,
        in_specs=[whole()] + [whole(pltpu.HBM)] * CORES,
        out_specs=[whole()] * (1 + CORES),
        out_shape=[pltpu.VMEM((xs, n_rows, width), jnp.bfloat16)]
        + [pltpu.VMEM(weight.shape, weight.dtype) for weight in weights],
        scratch_shapes=[pltpu.SemaphoreType.DMA((CORES,))],
    )(*near_memory(sums), *far_weights)


def down_kernel(*refs):
    passed, units, own, other, out = refs[:-4], *refs[-4:]
    near, _, block, _ = out.shape
    xs, _, width = units.shape
    x, core = lax.axis_index("x"), lax.axis_index("core")
    left = jnp.concatenate([ref[...] for ref in passed] + [units[n] for n in range(xs)], axis=1)
    starts = [lax.rem(x + (xs - shift), xs) * CORES + core for shift in range(xs)]
    starts += [number * CORES + (1 - core) for number in range(xs)]
    starts = [pl.multiple_of(start * width, width) for start in starts]
    for side, weight in ((core, own), (1 - core, other)):
        right = jnp.concatenate([weight[pl.ds(start, width), :] for start in starts], axis=0)
        product = jnp.dot(left, right, preferred_element_type=jnp.float32).astype(out.dtype)
        for line in range(near):
            out[line, side] = product[line * block : (line + 1) * block]


def down(passed, units, own, other, near):
    n_rows = units.shape[1]
    return pl.pallas_call(
        down_kernel,
        compiler_params=PARAMS,
        in_specs=[whole()] * (len(passed) + 3),
        out_specs=whole(),
        out_shape=pltpu.VMEM((near, CORES, n_rows // near, own.shape[1]), jnp.bfloat16),
    )(*near_memory(*passed, units, own, other))


def layer(tokens, route_ids, route_gates, gate_weight, up_weight, down_weight):
    f32, bf16 = jnp.float32, jnp.bfloat16
    model_width = tokens.shape[1]
    far, near, xs = lax.axis_size("far"), lax.axis_size("near"), lax.axis_size("x")
    x = lax.axis_index("x")
    chip_width = model_width // xs
    out_width = down_weight.shape[1]
    copies = far // EXPERTS
    swap = [(i, (i + 1) % CORES) for i in range(CORES)]
    sent, combine, residual = pack(tokens, route_ids, route_gates, far, chip_width, out_width)
    arrived = lax.all_to_all(sent, "far", 0, 0, tiled=True)

    def chunk(shift):
        start = (x + shift) % xs * chip_width
        return jnp.stack(
            [
                lax.dynamic_slice_in_dim(weight, start, chip_width, 0)
                for weight in (gate_weight, up_weight)
            ]
        )

    chunks = [chunk(0)]
    for shift in range(1, xs):
        chunks.append(lax.ppermute(chunk(shift), "x", [(i, (i + shift) % xs) for i in range(xs)]))
    down_other = lax.ppermute(down_weight, "core", swap)

    arrived = arrived.reshape(far, 2, PART, chip_width // 2)
    arrived = jnp.swapaxes(arrived, 1, 2).reshape(far * PART, chip_width)
    rows = lax.all_gather(arrived, "near", axis=0, tiled=True)
    rows, down_other = lax.optimization_barrier((rows, down_other))
    mine, stacked = own_products(rows, chunks)
    mine = lax.all_to_all(mine, "x", 0, 0, tiled=True)
    stacked = lax.ppermute(stacked, "core", swap)
    theirs = other_products(rows, stacked)
    theirs = lax.all_to_all(theirs, "x", 0, 0, tiled=True)
    ready = first_units(mine)
    passed = [ready]
    for shift in range(1, xs):
        passed.append(lax.ppermute(ready, "x", [(i, (i + shift) % xs) for i in range(xs)]))
    theirs, *passed = lax.optimization_barrier((theirs, *passed))
    hidden, down_weight, down_other = hidden_units(theirs, down_weight, down_other)
    units = lax.all_to_all(hidden, "x", 0, 0, tiled=True)
    produced = down(passed, units, down_weight, down_other, near)
    parts = lax.all_to_all(
        produced.reshape(near * CORES, far * PART, out_width), ("near", "core"), 0, 0, tiled=True
    )
    summed = jnp.sum(
        parts.reshape(near, CORES, far, PART, out_width).astype(f32), axis=0
    ).astype(bf16)
    summed = jnp.swapaxes(summed, 0, 1).reshape(far, CAP, out_width)
    returned = lax.all_to_all(summed, "far", 0, 0, tiled=True)
    returned = jnp.sum(
        returned.reshape(EXPERTS, copies, CAP, out_width).astype(f32), axis=1
    ).reshape(EXPERTS * CAP, out_width)
    mixture = jnp.einsum(
        "st,sd->td",
        combine,
        returned,
        precision=lax.Precision.HIGHEST,
        preferred_element_type=f32,
    )
    return (residual.astype(f32) + mixture).astype(bf16)


def solution(mesh):
    groups, experts, tensor = (mesh.shape[n] for n in ("groups", "expert", "tensor"))
    fine = Mesh(
        mesh.devices.reshape(groups, experts // NEAR, NEAR, tensor // CORES, CORES),
        ("groups", "far", "near", "x", "core"),
    )
    tok = ("groups", "far", "near")
    in_specs = (
        P(tok, None),
        P(tok, None),
        P(tok, None),
        P(None, ("far", "near", "x", "core")),
        P(None, ("far", "near", "x", "core")),
        P(("far", "near"), ("x", "core")),
    )
    out_specs = P(tok, ("x", "core"))
    return jax.shard_map(layer, mesh=fine, in_specs=in_specs, out_specs=out_specs, check_vma=False)
```

```python
import jax
import jax.numpy as jnp
from jax import lax
from jax.experimental import pallas as pl
from jax.experimental.pallas import tpu as pltpu
from jax.sharding import Mesh, PartitionSpec as P


EXPERTS = 4
CAP = 24
NEAR = 4
CORES = 2
PART = CAP // CORES

EPSILON = 1e-05


def whole(space=None):
    return pl.BlockSpec(memory_space=space or pltpu.VMEM)


PARAMS = pltpu.CompilerParams(vmem_limit_bytes=16 << 20)


def near_memory(*arrays):
    return [pltpu.with_memory_space_constraint(array, pltpu.VMEM) for array in arrays]


def pack_kernel(*refs):
    sources, (packed, combine, residual), held, sems = refs[:3], refs[3:6], refs[6:9], refs[9]
    moves = [
        pltpu.make_async_copy(source, place, sems.at[number])
        for number, (source, place) in enumerate(zip(sources, held))
    ]
    for move in moves:
        move.start()
    for move in moves:
        move.wait()
    tokens, ids, gates = held
    f32, bf16 = jnp.float32, jnp.bfloat16
    half = packed.shape[2]
    rows = tokens.shape[0]
    x, core = lax.axis_index("x"), lax.axis_index("core")
    out_width = residual.shape[1]
    floats = tokens[...].astype(f32)
    scale = lax.rsqrt(jnp.mean(floats * floats, axis=1, keepdims=True) + EPSILON)
    before = jnp.where(
        lax.broadcasted_iota(jnp.int32, (rows, rows), 0)
        < lax.broadcasted_iota(jnp.int32, (rows, rows), 1),
        1.0,
        0.0,
    ).astype(bf16)
    lines = EXPERTS * CAP
    line = lax.broadcasted_iota(jnp.int32, (lines, rows), 0)
    expert = sum((line >= CAP * e).astype(jnp.int32) for e in range(1, EXPERTS))
    at = line - expert * CAP
    first = ids[0:1, :] == expert
    second = ids[1:2, :] == expert
    named = jnp.where(jnp.logical_or(first, second), 1.0, 0.0)
    position = jnp.dot(named.astype(bf16), before, preferred_element_type=f32)
    gate = jnp.where(first, gates[0:1, :], jnp.where(second, gates[1:2, :], 0.0))
    combine[...] = jnp.where(position == at.astype(f32), gate, 0.0)
    upper = (at >= PART).astype(jnp.int32)
    wanted = (at - upper * PART + core * PART).astype(f32)
    picker = jnp.where(position == wanted, named, 0.0)
    total = jnp.zeros((lines, half), f32)
    for part in range(2):
        start = pl.multiple_of((x * 2 + part) * half, half)
        normed = (tokens[:, pl.ds(start, half)].astype(f32) * scale).astype(bf16)
        mine = jnp.where(upper == part, picker, 0.0).astype(bf16)
        total = total + jnp.dot(mine, normed, preferred_element_type=f32)
    total = total.astype(bf16)
    copies = packed.shape[0] // EXPERTS
    for e in range(EXPERTS):
        for copy in range(copies):
            packed[e * copies + copy] = total[e * CAP : (e + 1) * CAP]
    start = pl.multiple_of((x * CORES + core) * out_width, out_width)
    residual[...] = tokens[:, pl.ds(start, out_width)]


def pack(tokens, ids, gates, far, chip_width, out_width):
    rows = tokens.shape[0]
    arrays = (tokens, ids.T, gates.T)
    return pl.pallas_call(
        pack_kernel,
        compiler_params=PARAMS,
        in_specs=[whole(pltpu.HBM)] * 3,
        out_specs=[whole()] * 3,
        out_shape=[
            pltpu.VMEM((far, CAP, chip_width // 2), jnp.bfloat16),
            pltpu.VMEM((EXPERTS * CAP, rows), jnp.float32),
            pltpu.VMEM((rows, out_width), jnp.bfloat16),
        ],
        scratch_shapes=[pltpu.VMEM(array.shape, array.dtype) for array in arrays]
        + [pltpu.SemaphoreType.DMA((3,))],
    )(*[pltpu.with_memory_space_constraint(array, pltpu.HBM) for array in arrays])


def product_kernel(rows, *refs):
    xs = refs[-1].shape[0] + 1
    own, late, other, out = refs[:xs], refs[xs], refs[xs + 1 : 2 * xs], refs[2 * xs]
    held, sems = list(refs[2 * xs + 1 : -1]), refs[-1]
    moves = [
        pltpu.make_async_copy(source, place, sems.at[number])
        for number, (source, place) in enumerate(zip(other, held))
    ]
    for move in moves:
        move.start()
    held.insert(xs // 2, late)
    x = lax.axis_index("x")
    left = rows[...]
    width = out.shape[-1]
    for core, chunks in enumerate((own, held)):
        if core:
            for move in moves:
                move.wait()
        for shift in range(xs):
            to = lax.rem(x + (xs - shift), xs)
            both = jnp.concatenate([chunks[shift][kind] for kind in range(2)], axis=1)
            product = jnp.dot(left, both, preferred_element_type=jnp.float32).astype(out.dtype)
            for kind in range(2):
                out[to, core, kind] = product[:, kind * width : (kind + 1) * width]


def products(rows, own, other):
    n_rows, xs = rows.shape[0], len(own)
    width = own[0].shape[2]
    late = other[xs // 2]
    other = [
        pltpu.with_memory_space_constraint(chunk, pltpu.HBM)
        for shift, chunk in enumerate(other)
        if shift != xs // 2
    ]
    return pl.pallas_call(
        product_kernel,
        compiler_params=PARAMS,
        in_specs=[whole()] * (2 + xs) + [whole(pltpu.HBM)] * len(other),
        out_specs=whole(),
        out_shape=pltpu.VMEM((xs, CORES, 2, n_rows, width), jnp.bfloat16),
        scratch_shapes=[pltpu.VMEM(chunk.shape, chunk.dtype) for chunk in other]
        + [pltpu.SemaphoreType.DMA((len(other),))],
    )(*near_memory(rows, *own, late), *other)


def hidden_kernel(sums, *refs):
    sources, out, places, sems = refs[:CORES], refs[CORES], refs[CORES + 1 : -1], refs[-1]
    moves = [
        pltpu.make_async_copy(source, place, sems.at[number])
        for number, (source, place) in enumerate(zip(sources, places))
    ]
    for move in moves:
        move.start()
    f32 = jnp.float32
    xs, _, _, n_rows, width = sums.shape
    straight = lax.axis_index("core") == 0
    block = 32
    for at in range(0, n_rows, block):
        total = sums[0, :, :, at : at + block, :].astype(f32)
        for source in range(1, xs):
            total = total + sums[source, :, :, at : at + block, :].astype(f32)
        gate, up = total[:, 0], total[:, 1]
        hidden = (gate / (1.0 + jnp.exp(-gate)) * up).astype(out.dtype)
        low = jnp.where(straight, hidden[0], hidden[1])
        high = jnp.where(straight, hidden[1], hidden[0])
        for copy in range(out.shape[0]):
            out[copy, at : at + block, 0:width] = low
            out[copy, at : at + block, width : 2 * width] = high
    for move in moves:
        move.wait()


def hidden_units(sums, *weights):
    xs, cores, _, n_rows, width = sums.shape
    far_weights = [pltpu.with_memory_space_constraint(weight, pltpu.HBM) for weight in weights]
    return pl.pallas_call(
        hidden_kernel,
        compiler_params=PARAMS,
        in_specs=[whole()] + [whole(pltpu.HBM)] * CORES,
        out_specs=[whole()] * (1 + CORES),
        out_shape=[pltpu.VMEM((xs, n_rows, cores * width), jnp.bfloat16)]
        + [pltpu.VMEM(weight.shape, weight.dtype) for weight in weights],
        scratch_shapes=[pltpu.SemaphoreType.DMA((CORES,))],
    )(*near_memory(sums), *far_weights)


def down_kernel(units, own, other, out):
    near, _, block, _ = out.shape
    core = lax.axis_index("core")
    left = jnp.concatenate([units[source] for source in range(units.shape[0])], axis=1)
    for side, weight in ((core, own), (1 - core, other)):
        product = jnp.dot(left, weight[...], preferred_element_type=jnp.float32).astype(out.dtype)
        for line in range(near):
            out[line, side] = product[line * block : (line + 1) * block]


def down(units, own, other, near):
    n_rows = units.shape[1]
    return pl.pallas_call(
        down_kernel,
        compiler_params=PARAMS,
        in_specs=[whole()] * 3,
        out_specs=whole(),
        out_shape=pltpu.VMEM((near, CORES, n_rows // near, own.shape[1]), jnp.bfloat16),
    )(*near_memory(units, own, other))


def layer(tokens, route_ids, route_gates, gate_weight, up_weight, down_weight):
    f32, bf16 = jnp.float32, jnp.bfloat16
    model_width = tokens.shape[1]
    far, near, xs = lax.axis_size("far"), lax.axis_size("near"), lax.axis_size("x")
    x = lax.axis_index("x")
    chip_width = model_width // xs
    out_width = down_weight.shape[1]
    copies = far // EXPERTS
    swap = [(i, (i + 1) % CORES) for i in range(CORES)]
    sent, combine, residual = pack(tokens, route_ids, route_gates, far, chip_width, out_width)
    arrived = lax.all_to_all(sent, "far", 0, 0, tiled=True)

    def chunk(shift):
        start = (x + shift) % xs * chip_width
        return jnp.stack(
            [
                lax.dynamic_slice_in_dim(weight, start, chip_width, 0)
                for weight in (gate_weight, up_weight)
            ]
        )

    chunks = [chunk(0)]
    for shift in range(1, xs):
        chunks.append(lax.ppermute(chunk(shift), "x", [(i, (i + shift) % xs) for i in range(xs)]))
    swapped = []
    for shift in range(xs):
        swapped.append(lax.ppermute(chunks[shift], "core", swap))
    down_other = lax.ppermute(down_weight, "core", swap)

    arrived = arrived.reshape(far, 2, PART, chip_width // 2)
    arrived = jnp.swapaxes(arrived, 1, 2).reshape(far * PART, chip_width)
    rows = lax.all_gather(arrived, "near", axis=0, tiled=True)
    rows, down_other = lax.optimization_barrier((rows, down_other))
    partial = products(rows, chunks, swapped)
    sums = lax.all_to_all(partial, "x", 0, 0, tiled=True)
    hidden, down_weight, down_other = hidden_units(sums, down_weight, down_other)
    units = lax.all_to_all(hidden, "x", 0, 0, tiled=True)
    produced = down(units, down_weight, down_other, near)
    parts = lax.all_to_all(
        produced.reshape(near * CORES, far * PART, out_width), ("near", "core"), 0, 0, tiled=True
    )
    summed = jnp.sum(
        parts.reshape(near, CORES, far, PART, out_width).astype(f32), axis=0
    ).astype(bf16)
    summed = jnp.swapaxes(summed, 0, 1).reshape(far, CAP, out_width)
    returned = lax.all_to_all(summed, "far", 0, 0, tiled=True)
    returned = jnp.sum(
        returned.reshape(EXPERTS, copies, CAP, out_width).astype(f32), axis=1
    ).reshape(EXPERTS * CAP, out_width)
    mixture = jnp.einsum(
        "st,sd->td",
        combine,
        returned,
        precision=lax.Precision.HIGHEST,
        preferred_element_type=f32,
    )
    return (residual.astype(f32) + mixture).astype(bf16)


def solution(mesh):
    groups, experts, tensor = (mesh.shape[n] for n in ("groups", "expert", "tensor"))
    fine = Mesh(
        mesh.devices.reshape(groups, experts // NEAR, NEAR, tensor // CORES, CORES),
        ("groups", "far", "near", "x", "core"),
    )
    tok = ("groups", "far", "near")
    in_specs = (
        P(tok, None),
        P(tok, None),
        P(tok, None),
        P(None, ("far", "near", "x", "core")),
        P(None, ("far", "near", "x", "core")),
        P(("far", "near"), ("x", "core")),
    )
    out_specs = P(tok, ("x", "core"))
    return jax.shard_map(layer, mesh=fine, in_specs=in_specs, out_specs=out_specs, check_vma=False)
```

```python
import jax
import jax.numpy as jnp
from jax import lax
from jax.experimental import pallas as pl
from jax.experimental.pallas import tpu as pltpu
from jax.sharding import Mesh, PartitionSpec as P


EXPERTS = 4
CAP = 24
NEAR = 4
CORES = 2
PART = CAP // CORES

EPSILON = 1e-05


def whole(space=None):
    return pl.BlockSpec(memory_space=space or pltpu.VMEM)


PARAMS = pltpu.CompilerParams(vmem_limit_bytes=16 << 20)


def near_memory(*arrays):
    return [pltpu.with_memory_space_constraint(array, pltpu.VMEM) for array in arrays]


def pack_kernel(*refs):
    sources, (packed, combine, residual), held, sems = refs[:3], refs[3:6], refs[6:9], refs[9]
    moves = [
        pltpu.make_async_copy(source, place, sems.at[number])
        for number, (source, place) in enumerate(zip(sources, held))
    ]
    for move in moves:
        move.start()
    moves[0].wait()
    tokens, ids, gates = held
    f32, bf16 = jnp.float32, jnp.bfloat16
    half = packed.shape[2]
    rows = tokens.shape[0]
    x, core = lax.axis_index("x"), lax.axis_index("core")
    out_width = residual.shape[1]
    floats = tokens[...].astype(f32)
    scale = lax.rsqrt(jnp.mean(floats * floats, axis=1, keepdims=True) + EPSILON)
    for move in moves[1:]:
        move.wait()
    before = jnp.where(
        lax.broadcasted_iota(jnp.int32, (rows, rows), 0)
        < lax.broadcasted_iota(jnp.int32, (rows, rows), 1),
        1.0,
        0.0,
    ).astype(bf16)
    lines = EXPERTS * CAP
    line = lax.broadcasted_iota(jnp.int32, (lines, rows), 0)
    expert = sum((line >= CAP * e).astype(jnp.int32) for e in range(1, EXPERTS))
    at = line - expert * CAP
    first = ids[0:1, :] == expert
    second = ids[1:2, :] == expert
    named = jnp.where(jnp.logical_or(first, second), 1.0, 0.0)
    position = jnp.dot(named.astype(bf16), before, preferred_element_type=f32)
    gate = jnp.where(first, gates[0:1, :], jnp.where(second, gates[1:2, :], 0.0))
    combine[...] = jnp.where(position == at.astype(f32), gate, 0.0)
    upper = (at >= PART).astype(jnp.int32)
    wanted = (at - upper * PART + core * PART).astype(f32)
    picker = jnp.where(position == wanted, named, 0.0)
    total = jnp.zeros((lines, half), f32)
    for part in range(2):
        start = pl.multiple_of((x * 2 + part) * half, half)
        normed = (tokens[:, pl.ds(start, half)].astype(f32) * scale).astype(bf16)
        mine = jnp.where(upper == part, picker, 0.0).astype(bf16)
        total = total + jnp.dot(mine, normed, preferred_element_type=f32)
    total = total.astype(bf16)
    copies = packed.shape[0] // EXPERTS
    for e in range(EXPERTS):
        for copy in range(copies):
            packed[e * copies + copy] = total[e * CAP : (e + 1) * CAP]
    start = pl.multiple_of((x * CORES + core) * out_width, out_width)
    residual[...] = tokens[:, pl.ds(start, out_width)]


def pack(tokens, ids, gates, far, chip_width, out_width):
    rows = tokens.shape[0]
    arrays = (tokens, ids.T, gates.T)
    return pl.pallas_call(
        pack_kernel,
        compiler_params=PARAMS,
        in_specs=[whole(pltpu.HBM)] * 3,
        out_specs=[whole()] * 3,
        out_shape=[
            pltpu.VMEM((far, CAP, chip_width // 2), jnp.bfloat16),
            pltpu.VMEM((EXPERTS * CAP, rows), jnp.float32),
            pltpu.VMEM((rows, out_width), jnp.bfloat16),
        ],
        scratch_shapes=[pltpu.VMEM(array.shape, array.dtype) for array in arrays]
        + [pltpu.SemaphoreType.DMA((3,))],
    )(*[pltpu.with_memory_space_constraint(array, pltpu.HBM) for array in arrays])


def product_kernel(rows, own, other, out, held, sem):
    xs, kinds, _, width = own.shape
    half = xs // 2
    moves = [
        pltpu.make_async_copy(
            other.at[pl.ds(part * half, half)], held.at[pl.ds(part * half, half)], sem.at[part]
        )
        for part in range(2)
    ]
    for move in moves:
        move.start()
    x = lax.axis_index("x")
    left = rows[...]
    for core, weights in enumerate((own, held)):
        for shift in range(xs):
            if core and shift % half == 0:
                moves[shift // half].wait()
            to = lax.rem(x + (xs - shift), xs)
            both = jnp.concatenate([weights[shift, kind] for kind in range(kinds)], axis=1)
            product = jnp.dot(left, both, preferred_element_type=jnp.float32).astype(out.dtype)
            for kind in range(kinds):
                out[to, core, kind] = product[:, kind * width : (kind + 1) * width]


def products(rows, own, other):
    n_rows = rows.shape[0]
    xs, kinds, _, width = own.shape
    return pl.pallas_call(
        product_kernel,
        compiler_params=PARAMS,
        in_specs=[whole(), whole(), whole(pltpu.HBM)],
        out_specs=whole(),
        out_shape=pltpu.VMEM((xs, CORES, kinds, n_rows, width), jnp.bfloat16),
        scratch_shapes=[pltpu.VMEM(other.shape, other.dtype), pltpu.SemaphoreType.DMA((2,))],
    )(*near_memory(rows, own), pltpu.with_memory_space_constraint(other, pltpu.HBM))


def hidden_kernel(sums, *refs):
    sources, out, places, sems = refs[:CORES], refs[CORES], refs[CORES + 1 : -1], refs[-1]
    moves = [
        pltpu.make_async_copy(source, place, sems.at[number])
        for number, (source, place) in enumerate(zip(sources, places))
    ]
    for move in moves:
        move.start()
    f32 = jnp.float32
    xs, _, _, n_rows, width = sums.shape
    straight = lax.axis_index("core") == 0
    block = 32
    for at in range(0, n_rows, block):
        total = sums[0, :, :, at : at + block, :].astype(f32)
        for source in range(1, xs):
            total = total + sums[source, :, :, at : at + block, :].astype(f32)
        gate, up = total[:, 0], total[:, 1]
        hidden = (gate / (1.0 + jnp.exp(-gate)) * up).astype(out.dtype)
        low = jnp.where(straight, hidden[0], hidden[1])
        high = jnp.where(straight, hidden[1], hidden[0])
        for copy in range(out.shape[0]):
            out[copy, at : at + block, 0:width] = low
            out[copy, at : at + block, width : 2 * width] = high
    for move in moves:
        move.wait()


def hidden_units(sums, *weights):
    xs, cores, _, n_rows, width = sums.shape
    far_weights = [pltpu.with_memory_space_constraint(weight, pltpu.HBM) for weight in weights]
    return pl.pallas_call(
        hidden_kernel,
        compiler_params=PARAMS,
        in_specs=[whole()] + [whole(pltpu.HBM)] * CORES,
        out_specs=[whole()] * (1 + CORES),
        out_shape=[pltpu.VMEM((xs, n_rows, cores * width), jnp.bfloat16)]
        + [pltpu.VMEM(weight.shape, weight.dtype) for weight in weights],
        scratch_shapes=[pltpu.SemaphoreType.DMA((CORES,))],
    )(*near_memory(sums), *far_weights)


def down_kernel(units, own, other, out):
    near, _, block, _ = out.shape
    core = lax.axis_index("core")
    left = jnp.concatenate([units[source] for source in range(units.shape[0])], axis=1)
    for side, weight in ((core, own), (1 - core, other)):
        product = jnp.dot(left, weight[...], preferred_element_type=jnp.float32).astype(out.dtype)
        for line in range(near):
            out[line, side] = product[line * block : (line + 1) * block]


def down(units, own, other, near):
    n_rows = units.shape[1]
    return pl.pallas_call(
        down_kernel,
        compiler_params=PARAMS,
        in_specs=[whole()] * 3,
        out_specs=whole(),
        out_shape=pltpu.VMEM((near, CORES, n_rows // near, own.shape[1]), jnp.bfloat16),
    )(*near_memory(units, own, other))


def layer(tokens, route_ids, route_gates, gate_weight, up_weight, down_weight):
    f32, bf16 = jnp.float32, jnp.bfloat16
    model_width = tokens.shape[1]
    far, near, xs = lax.axis_size("far"), lax.axis_size("near"), lax.axis_size("x")
    x = lax.axis_index("x")
    chip_width = model_width // xs
    out_width = down_weight.shape[1]
    copies = far // EXPERTS
    swap = [(i, (i + 1) % CORES) for i in range(CORES)]
    sent, combine, residual = pack(tokens, route_ids, route_gates, far, chip_width, out_width)
    arrived = lax.all_to_all(sent, "far", 0, 0, tiled=True)

    def chunk(shift):
        start = (x + shift) % xs * chip_width
        return jnp.stack(
            [
                lax.dynamic_slice_in_dim(weight, start, chip_width, 0)
                for weight in (gate_weight, up_weight)
            ]
        )

    chunks = [chunk(0)]
    for shift in range(1, xs):
        chunks.append(lax.ppermute(chunk(shift), "x", [(i, (i + shift) % xs) for i in range(xs)]))
    own = jnp.stack(chunks)
    other = lax.ppermute(own, "core", swap)
    down_other = lax.ppermute(down_weight, "core", swap)

    arrived = arrived.reshape(far, 2, PART, chip_width // 2)
    arrived = jnp.swapaxes(arrived, 1, 2).reshape(1, far * PART, chip_width)
    rows = lax.all_to_all(
        jnp.broadcast_to(arrived, (near, far * PART, chip_width)), "near", 0, 0, tiled=True
    )
    n_rows = near * far * PART
    rows, down_other = lax.optimization_barrier((rows, down_other))
    partial = products(rows.reshape(n_rows, chip_width), own, other)
    sums = lax.all_to_all(partial, "x", 0, 0, tiled=True)
    hidden, down_weight, down_other = hidden_units(sums, down_weight, down_other)
    units = lax.all_to_all(hidden, "x", 0, 0, tiled=True)
    produced = down(units, down_weight, down_other, near)
    parts = lax.all_to_all(
        produced.reshape(near * CORES, far * PART, out_width), ("near", "core"), 0, 0, tiled=True
    )
    summed = jnp.sum(
        parts.reshape(near, CORES, far, PART, out_width).astype(f32), axis=0
    ).astype(bf16)
    summed = jnp.swapaxes(summed, 0, 1).reshape(far, CAP, out_width)
    returned = lax.all_to_all(summed, "far", 0, 0, tiled=True)
    returned = jnp.sum(
        returned.reshape(EXPERTS, copies, CAP, out_width).astype(f32), axis=1
    ).reshape(EXPERTS * CAP, out_width)
    mixture = jnp.einsum(
        "st,sd->td",
        combine,
        returned,
        precision=lax.Precision.HIGHEST,
        preferred_element_type=f32,
    )
    return (residual.astype(f32) + mixture).astype(bf16)


def solution(mesh):
    groups, experts, tensor = (mesh.shape[n] for n in ("groups", "expert", "tensor"))
    fine = Mesh(
        mesh.devices.reshape(groups, experts // NEAR, NEAR, tensor // CORES, CORES),
        ("groups", "far", "near", "x", "core"),
    )
    tok = ("groups", "far", "near")
    in_specs = (
        P(tok, None),
        P(tok, None),
        P(tok, None),
        P(None, ("far", "near", "x", "core")),
        P(None, ("far", "near", "x", "core")),
        P(("far", "near"), ("x", "core")),
    )
    out_specs = P(tok, ("x", "core"))
    return jax.shard_map(layer, mesh=fine, in_specs=in_specs, out_specs=out_specs, check_vma=False)
```

```python
import jax
import jax.numpy as jnp
from jax import lax
from jax.experimental import pallas as pl
from jax.experimental.pallas import tpu as pltpu
from jax.sharding import Mesh, PartitionSpec as P


EXPERTS = 4
CAP = 24
NEAR = 2
CORES = 2
PART = CAP // CORES

EPSILON = 1e-05


def whole(space=None):
    return pl.BlockSpec(memory_space=space or pltpu.VMEM)


PARAMS = pltpu.CompilerParams(vmem_limit_bytes=16 << 20)


def near_memory(*arrays):
    return [pltpu.with_memory_space_constraint(array, pltpu.VMEM) for array in arrays]


def pack_kernel(*refs):
    sources, (packed, combine, residual), held, sems = refs[:3], refs[3:6], refs[6:9], refs[9]
    moves = [
        pltpu.make_async_copy(source, place, sems.at[number])
        for number, (source, place) in enumerate(zip(sources, held))
    ]
    for move in moves:
        move.start()
    for move in moves:
        move.wait()
    tokens, ids, gates = held
    f32, bf16 = jnp.float32, jnp.bfloat16
    half = packed.shape[2]
    rows = tokens.shape[0]
    x, core = lax.axis_index("x"), lax.axis_index("core")
    out_width = residual.shape[1]
    floats = tokens[...].astype(f32)
    scale = lax.rsqrt(jnp.mean(floats * floats, axis=1, keepdims=True) + EPSILON)
    before = jnp.where(
        lax.broadcasted_iota(jnp.int32, (rows, rows), 0)
        < lax.broadcasted_iota(jnp.int32, (rows, rows), 1),
        1.0,
        0.0,
    ).astype(bf16)
    lines = EXPERTS * CAP
    line = lax.broadcasted_iota(jnp.int32, (lines, rows), 0)
    expert = sum((line >= CAP * e).astype(jnp.int32) for e in range(1, EXPERTS))
    at = line - expert * CAP
    first = ids[0:1, :] == expert
    second = ids[1:2, :] == expert
    named = jnp.where(jnp.logical_or(first, second), 1.0, 0.0)
    position = jnp.dot(named.astype(bf16), before, preferred_element_type=f32)
    gate = jnp.where(first, gates[0:1, :], jnp.where(second, gates[1:2, :], 0.0))
    combine[...] = jnp.where(position == at.astype(f32), gate, 0.0)
    upper = (at >= PART).astype(jnp.int32)
    wanted = (at - upper * PART + core * PART).astype(f32)
    picker = jnp.where(position == wanted, named, 0.0)
    total = jnp.zeros((lines, half), f32)
    for part in range(2):
        start = pl.multiple_of((x * 2 + part) * half, half)
        normed = (tokens[:, pl.ds(start, half)].astype(f32) * scale).astype(bf16)
        mine = jnp.where(upper == part, picker, 0.0).astype(bf16)
        total = total + jnp.dot(mine, normed, preferred_element_type=f32)
    total = total.astype(bf16)
    copies = packed.shape[0] // EXPERTS
    for e in range(EXPERTS):
        for copy in range(copies):
            packed[e * copies + copy] = total[e * CAP : (e + 1) * CAP]
    start = pl.multiple_of((x * CORES + core) * out_width, out_width)
    residual[...] = tokens[:, pl.ds(start, out_width)]


def pack(tokens, ids, gates, far, chip_width, out_width):
    rows = tokens.shape[0]
    arrays = (tokens, ids.T, gates.T)
    return pl.pallas_call(
        pack_kernel,
        compiler_params=PARAMS,
        in_specs=[whole(pltpu.HBM)] * 3,
        out_specs=[whole()] * 3,
        out_shape=[
            pltpu.VMEM((far, CAP, chip_width // 2), jnp.bfloat16),
            pltpu.VMEM((EXPERTS * CAP, rows), jnp.float32),
            pltpu.VMEM((rows, out_width), jnp.bfloat16),
        ],
        scratch_shapes=[pltpu.VMEM(array.shape, array.dtype) for array in arrays]
        + [pltpu.SemaphoreType.DMA((3,))],
    )(*[pltpu.with_memory_space_constraint(array, pltpu.HBM) for array in arrays])


def product_kernel(rows, own, other, out, held, sem):
    xs, kinds, _, width = own.shape
    move = pltpu.make_async_copy(other, held, sem)
    move.start()
    x = lax.axis_index("x")
    left = rows[...]
    for core, weights in enumerate((own, held)):
        if core:
            move.wait()
        for shift in range(xs):
            to = lax.rem(x + (xs - shift), xs)
            both = jnp.concatenate([weights[shift, kind] for kind in range(kinds)], axis=1)
            product = jnp.dot(left, both, preferred_element_type=jnp.float32).astype(out.dtype)
            for kind in range(kinds):
                out[to, core, kind] = product[:, kind * width : (kind + 1) * width]


def products(rows, own, other):
    n_rows = rows.shape[0]
    xs, kinds, _, width = own.shape
    return pl.pallas_call(
        product_kernel,
        compiler_params=PARAMS,
        in_specs=[whole(), whole(), whole(pltpu.HBM)],
        out_specs=whole(),
        out_shape=pltpu.VMEM((xs, CORES, kinds, n_rows, width), jnp.bfloat16),
        scratch_shapes=[pltpu.VMEM(other.shape, other.dtype), pltpu.SemaphoreType.DMA],
    )(*near_memory(rows, own), pltpu.with_memory_space_constraint(other, pltpu.HBM))


def hidden_kernel(sums, *refs):
    sources, out, places, sems = refs[:CORES], refs[CORES], refs[CORES + 1 : -1], refs[-1]
    moves = [
        pltpu.make_async_copy(source, place, sems.at[number])
        for number, (source, place) in enumerate(zip(sources, places))
    ]
    for move in moves:
        move.start()
    f32 = jnp.float32
    xs, _, _, n_rows, width = sums.shape
    straight = lax.axis_index("core") == 0
    block = 32
    for at in range(0, n_rows, block):
        total = sums[0, :, :, at : at + block, :].astype(f32)
        for source in range(1, xs):
            total = total + sums[source, :, :, at : at + block, :].astype(f32)
        gate, up = total[:, 0], total[:, 1]
        hidden = (gate / (1.0 + jnp.exp(-gate)) * up).astype(out.dtype)
        low = jnp.where(straight, hidden[0], hidden[1])
        high = jnp.where(straight, hidden[1], hidden[0])
        for copy in range(out.shape[0]):
            out[copy, at : at + block, 0:width] = low
            out[copy, at : at + block, width : 2 * width] = high
    for move in moves:
        move.wait()


def hidden_units(sums, *weights):
    xs, cores, _, n_rows, width = sums.shape
    far_weights = [pltpu.with_memory_space_constraint(weight, pltpu.HBM) for weight in weights]
    return pl.pallas_call(
        hidden_kernel,
        compiler_params=PARAMS,
        in_specs=[whole()] + [whole(pltpu.HBM)] * CORES,
        out_specs=[whole()] * (1 + CORES),
        out_shape=[pltpu.VMEM((xs, n_rows, cores * width), jnp.bfloat16)]
        + [pltpu.VMEM(weight.shape, weight.dtype) for weight in weights],
        scratch_shapes=[pltpu.SemaphoreType.DMA((CORES,))],
    )(*near_memory(sums), *far_weights)


def down_kernel(units, own, other, out):
    near, _, block, _ = out.shape
    core = lax.axis_index("core")
    left = jnp.concatenate([units[source] for source in range(units.shape[0])], axis=1)
    for side, weight in ((core, own), (1 - core, other)):
        product = jnp.dot(left, weight[...], preferred_element_type=jnp.float32).astype(out.dtype)
        for line in range(near):
            out[line, side] = product[line * block : (line + 1) * block]


def down(units, own, other, near):
    n_rows = units.shape[1]
    return pl.pallas_call(
        down_kernel,
        compiler_params=PARAMS,
        in_specs=[whole()] * 3,
        out_specs=whole(),
        out_shape=pltpu.VMEM((near, CORES, n_rows // near, own.shape[1]), jnp.bfloat16),
    )(*near_memory(units, own, other))


def layer(tokens, route_ids, route_gates, gate_weight, up_weight, down_weight):
    f32, bf16 = jnp.float32, jnp.bfloat16
    model_width = tokens.shape[1]
    far, near, xs = lax.axis_size("far"), lax.axis_size("near"), lax.axis_size("x")
    x = lax.axis_index("x")
    chip_width = model_width // xs
    out_width = down_weight.shape[1]
    copies = far // EXPERTS
    swap = [(i, (i + 1) % CORES) for i in range(CORES)]
    sent, combine, residual = pack(tokens, route_ids, route_gates, far, chip_width, out_width)
    arrived = lax.all_to_all(sent, "far", 0, 0, tiled=True)

    def chunk(shift):
        start = (x + shift) % xs * chip_width
        return jnp.stack(
            [
                lax.dynamic_slice_in_dim(weight, start, chip_width, 0)
                for weight in (gate_weight, up_weight)
            ]
        )

    chunks = [chunk(0)]
    for shift in range(1, xs):
        chunks.append(lax.ppermute(chunk(shift), "x", [(i, (i + shift) % xs) for i in range(xs)]))
    own = jnp.stack(chunks)
    other = lax.ppermute(own, "core", swap)
    down_other = lax.ppermute(down_weight, "core", swap)

    arrived = arrived.reshape(far, 2, PART, chip_width // 2)
    arrived = jnp.swapaxes(arrived, 1, 2).reshape(1, far * PART, chip_width)
    rows = lax.all_to_all(
        jnp.broadcast_to(arrived, (near, far * PART, chip_width)), "near", 0, 0, tiled=True
    )
    n_rows = near * far * PART
    rows, down_other = lax.optimization_barrier((rows, down_other))
    partial = products(rows.reshape(n_rows, chip_width), own, other)
    sums = lax.all_to_all(partial, "x", 0, 0, tiled=True)
    hidden, down_weight, down_other = hidden_units(sums, down_weight, down_other)
    units = lax.all_to_all(hidden, "x", 0, 0, tiled=True)
    produced = down(units, down_weight, down_other, near)
    parts = lax.all_to_all(
        produced.reshape(near * CORES, far * PART, out_width), ("near", "core"), 0, 0, tiled=True
    )
    summed = jnp.sum(
        parts.reshape(near, CORES, far, PART, out_width).astype(f32), axis=0
    ).astype(bf16)
    summed = jnp.swapaxes(summed, 0, 1).reshape(far, CAP, out_width)
    returned = lax.all_to_all(summed, "far", 0, 0, tiled=True)
    returned = jnp.sum(
        returned.reshape(EXPERTS, copies, CAP, out_width).astype(f32), axis=1
    ).reshape(EXPERTS * CAP, out_width)
    mixture = jnp.einsum(
        "st,sd->td",
        combine,
        returned,
        precision=lax.Precision.HIGHEST,
        preferred_element_type=f32,
    )
    return (residual.astype(f32) + mixture).astype(bf16)


def solution(mesh):
    groups, experts, tensor = (mesh.shape[n] for n in ("groups", "expert", "tensor"))
    fine = Mesh(
        mesh.devices.reshape(groups, experts // NEAR, NEAR, tensor // CORES, CORES),
        ("groups", "far", "near", "x", "core"),
    )
    tok = ("groups", "far", "near")
    in_specs = (
        P(tok, None),
        P(tok, None),
        P(tok, None),
        P(None, ("far", "near", "x", "core")),
        P(None, ("far", "near", "x", "core")),
        P(("far", "near"), ("x", "core")),
    )
    out_specs = P(tok, ("x", "core"))
    return jax.shard_map(layer, mesh=fine, in_specs=in_specs, out_specs=out_specs, check_vma=False)
```
